32 devices in a mesh: gx: 8 (over y, x, core), gy: 4 (over z).
Axes of the slice: x: 2, y: 2, z: 4, core: 2. Of those that a mesh axis runs over, the one named last changes fastest.
Arguments:
- coarse_source: float32 [256, 4096], P('gx', 'gy'), may hold values from -6 to 6
- coarse_coefficient: float32 [256, 4096], P('gx', 'gy'), may hold values from 0.25 to 4
- coarse_start: float32 [256, 4096], P('gx', 'gy'), may hold values from -6 to 6
- fine_source: float32 [32, 32, 1024], P(('gx', 'gy')), may hold values from -6 to 6
- fine_coefficient: float32 [32, 32, 1024], P(('gx', 'gy')), may hold values from 0.25 to 4
- fine_start: float32 [32, 32, 1024], P(('gx', 'gy')), may hold values from -6 to 6
- fine_position: int32 [32], replicated, may hold values from 0 to 255, as said below
- first_colour: int32 [3], replicated, may hold values from 0 to 1
Outputs:
- coarse_solution: float32 [256, 4096], P('gx', 'gy')
- fine_solution: float32 [32, 32, 1024], P(('gx', 'gy'))
The draws below stay inside these ranges and needn't reach their ends.
Inputs may be any that keep to these rules, and one draw needn't show every extreme that they name: `fine_position`: entry r is the box held by device r = gx index * 4 + gy index; its coarse device p // 8 has the same gy index as device r; only octants whose three bits sum to an even number occur, so no two boxes share a face; positions are distinct; in every gy index some coarse device lies under four boxes, and some box lies 8 // 2 gx indices away from its coarse device.
All inputs are finite; a program needn't handle non-finite values.
Results may differ from the reference program's by a relative error of at most 0.0003.
Values sent between devices are 32-bit elements; how exact they have to be, the bound alone decides.
No kernel may reach another device: no remote copies, remote signals or barrier semaphores. Data moves between devices by JAX's collectives and lax.ppermute only.
A program may use at most 64 MiB of HBM per device.

```python
import math
import jax
import jax.numpy as jnp
from jax import lax

B = 32
SWEEPS = 4
NCX = 256
NCY = 128
FBOXES = 32
N_GX = 8
N_GY = 4


def draw_fine_position(key, part):
    octant_kinds = jnp.array([0, 3, 5, 6], dtype=jnp.int32)

    def one_row(row_number):
        row_key = jax.random.fold_in(jax.random.fold_in(key, 7), row_number)
        crowded_x = jax.random.randint(jax.random.fold_in(row_key, 1), (), 0, N_GX)
        labels = jnp.arange(4 * (N_GX - 1), dtype=jnp.int32)
        shuffled = jax.random.permutation(jax.random.fold_in(row_key, 2), labels)
        chosen = shuffled[:N_GX - 4]
        column = chosen // 4
        column = column + (column >= crowded_x).astype(jnp.int32)
        octant = octant_kinds[chosen % 4]
        others = (column * N_GY + row_number) * 8 + octant
        crowded = (crowded_x * N_GY + row_number) * 8 + octant_kinds
        positions = jnp.concatenate([others, crowded]).astype(jnp.int32)
        columns = positions // 8 // N_GY
        holders = jax.random.permutation(jax.random.fold_in(row_key, 3), jnp.arange(N_GX, dtype=jnp.int32)).astype(jnp.int32)
        pick = jax.random.randint(jax.random.fold_in(row_key, 4), (), 0, N_GX).astype(jnp.int32)
        wanted = ((columns[pick] + N_GX // 2) % N_GX).astype(jnp.int32)
        indices = jnp.arange(N_GX, dtype=jnp.int32)
        spot = jnp.sum(jnp.where(holders == wanted, indices, 0)).astype(jnp.int32)
        previous = holders[pick]
        holders = holders.at[spot].set(previous)
        holders = holders.at[pick].set(wanted)
        return jnp.zeros((N_GX,), jnp.int32).at[holders].set(positions)
    table_rows = jax.vmap(one_row)(jnp.arange(N_GY, dtype=jnp.int32))
    return table_rows.T.reshape(N_GX * N_GY).astype(jnp.int32)


def level_of(key, extent, cuts, low, high):
    loudness = 1.0
    for dim, shards_of in cuts:
        heights = jax.random.uniform(jax.random.fold_in(jax.random.fold_in(key, 6), dim), (shards_of,), jnp.float32, low / len(cuts), high / len(cuts))
        loudness = loudness * jnp.repeat(jnp.exp(heights), extent[dim] // shards_of).reshape((-1,) + (1,) * (len(extent) - 1 - dim))
    return loudness


def noise(rng, shape, width, most, pieces=(), kind=jnp.bfloat16):
    result = jax.random.normal(rng, shape, jnp.float32) * width
    if len(pieces) > 0:
        result = level_of(rng, shape, pieces, -0.22, 0.18) * result
    return jnp.clip(result, min=-most, max=most).astype(kind)


def setup_inputs(seed: int = 0) -> dict:
    arg_keys = jax.random.split(jax.random.key(seed), 9)
    coarse_source = noise(arg_keys[0], (NCX, NCY * B), 1.0, 6.0, ((0, 8), (1, 4)), jnp.float32)
    coarse_coefficient = jnp.clip(jnp.exp(math.log(4.0) - 2.7725887 * jax.random.uniform(arg_keys[1], (NCX, NCY * B), jnp.float32) ** level_of(arg_keys[1], (NCX, NCY * B), ((0, 8), (1, 4)), -0.2, 0.2)), 0.25, 4.0)
    coarse_start = noise(arg_keys[2], (NCX, NCY * B), 1.0, 6.0, ((0, 8), (1, 4)), jnp.float32)
    fine_source = noise(arg_keys[3], (FBOXES, B, B * B), 1.0, 6.0, ((0, 32),), jnp.float32)
    fine_coefficient = jnp.clip(jnp.exp(math.log(4.0) - 2.7725887 * jax.random.uniform(arg_keys[4], (FBOXES, B, B * B), jnp.float32) ** level_of(arg_keys[4], (FBOXES, B, B * B), ((0, 32),), -0.2, 0.2)), 0.25, 4.0)
    fine_start = noise(arg_keys[5], (FBOXES, B, B * B), 1.0, 6.0, ((0, 32),), jnp.float32)
    fine_position = draw_fine_position(jax.random.fold_in(arg_keys[8], 71), 0)
    first_colour = jax.random.randint(arg_keys[7], (3,), 0, 2).astype(jnp.int32)
    return {"coarse_source": coarse_source, "coarse_coefficient": coarse_coefficient, "coarse_start": coarse_start, "fine_source": fine_source, "fine_coefficient": fine_coefficient, "fine_start": fine_start, "fine_position": fine_position, "first_colour": first_colour}


def shifted(values, stride, before, beyond):
    column = lax.broadcasted_iota(jnp.int32, values.shape, 1) % stride
    blanks = jnp.zeros_like(values[:, :1])
    toward = jnp.concatenate([blanks, values[:, :-1]], axis=1)
    backward = jnp.concatenate([values[:, 1:], blanks], axis=1)
    behind = jnp.where(column == 0, before, toward)
    forward = jnp.where(column == stride - 1, beyond, backward)
    return behind, forward


def neighbours(values, borders, stride, before, beyond):
    x_before, x_beyond, y_before, y_beyond = borders
    x_minus = jnp.concatenate([x_before, values[:-1]], axis=0)
    x_plus = jnp.concatenate([values[1:], x_beyond], axis=0)
    y_minus = jnp.concatenate([y_before, values[:, :-stride]], axis=1)
    y_plus = jnp.concatenate([values[:, stride:], y_beyond], axis=1)
    z_minus, z_plus = shifted(values, stride, before, beyond)
    return (x_minus, x_plus, y_minus, y_plus, z_minus, z_plus)


def face_terms(coefficient, around):
    weights = tuple(0.5 * (coefficient + neighbour) for neighbour in around)
    diagonal = weights[0] + weights[1] + weights[2] + weights[3] + weights[4] + weights[5]
    return weights, diagonal


def coupling(weights, around):
    total = weights[0] * around[0]
    for number in range(1, 6):
        total = total + weights[number] * around[number]
    return total


def relaxed(values, source, coupled, diagonal, factor, parity, colour):
    fresh = (source + factor * coupled) / (factor * diagonal)
    return jnp.where(parity == colour, fresh, values)


def residual_of(values, source, weights, diagonal, around, factor):
    return source - factor * (diagonal * values - coupling(weights, around))


def parity_of(rows_count, breadth, stride):
    along_x = lax.broadcasted_iota(jnp.int32, (rows_count, breadth), 0)
    flattened = lax.broadcasted_iota(jnp.int32, (rows_count, breadth), 1)
    return (along_x + flattened // stride + flattened % stride) % 2


def coarsen(values, stride):
    rows_count = values.shape[0]
    planes = values.shape[1] // stride
    volume = values.reshape(rows_count // 2, 2, planes // 2, 2, stride // 2, 2)
    summed = volume[:, 0] + volume[:, 1]
    summed = summed[:, :, 0] + summed[:, :, 1]
    summed = summed[..., 0] + summed[..., 1]
    return (0.125 * summed).reshape(rows_count // 2, (planes // 2) * (stride // 2))


def refine(values, stride):
    rows_count = values.shape[0]
    planes = values.shape[1] // stride
    volume = values.reshape(rows_count, planes, stride)
    volume = jnp.repeat(jnp.repeat(jnp.repeat(volume, 2, axis=0), 2, axis=1), 2, axis=2)
    return volume.reshape(2 * rows_count, 4 * planes * stride)


def enlarge(surface):
    return jnp.repeat(jnp.repeat(surface, 2, axis=0), 2, axis=1)


def zero_borders(values, stride):
    blank_row = jnp.zeros_like(values[:1])
    blank_side = jnp.zeros_like(values[:, :stride])
    return (blank_row, blank_row, blank_side, blank_side)


def fine_sweep(surfaces, source, coefficient, start, leading, parity, box_edge):
    widened = [enlarge(surface) for surface in surfaces]
    ghosts = (widened[0].reshape(1, box_edge * box_edge), widened[1].reshape(1, box_edge * box_edge), widened[2], widened[3])
    ghost_before = jnp.repeat(widened[4], box_edge, axis=1)
    ghost_beyond = jnp.repeat(widened[5], box_edge, axis=1)
    inside = (coefficient[:1], coefficient[-1:], coefficient[:, :box_edge], coefficient[:, -box_edge:])
    weights, diagonal = face_terms(coefficient, neighbours(coefficient, inside, box_edge, coefficient, coefficient))
    values = start
    for colour in (leading, 1 - leading):
        coupled = coupling(weights, neighbours(values, ghosts, box_edge, ghost_before, ghost_beyond))
        values = relaxed(values, source, coupled, diagonal, 4.0, parity, colour)
    remainder = residual_of(values, source, weights, diagonal, neighbours(values, ghosts, box_edge, ghost_before, ghost_beyond), 4.0)
    return values, coarsen(remainder, box_edge)


def bottom_sweeps(source, weights, diagonal, parity, leading, borders_of, half_edge):
    values = jnp.zeros_like(source)
    started = False
    for passage in range(SWEEPS):
        for colour in (leading, 1 - leading):
            if started:
                coupled = coupling(weights, neighbours(values, borders_of(values), half_edge, 0.0, 0.0))
            else:
                coupled = jnp.zeros_like(values)
            started = True
            values = relaxed(values, source, coupled, diagonal, 0.25, parity, colour)
    return values


def reference(coarse_source, coarse_coefficient, coarse_start, fine_source, fine_coefficient, fine_start, fine_position, first_colour):
    box_edge = B
    half_edge = B // 2
    outside = zero_borders(coarse_start, box_edge)
    parity_coarse = parity_of(NCX, NCY * box_edge, box_edge)
    weights_c, diagonal_c = face_terms(coarse_coefficient, neighbours(coarse_coefficient, outside, box_edge, 0.0, 0.0))
    resid_c = residual_of(coarse_start, coarse_source, weights_c, diagonal_c, neighbours(coarse_start, outside, box_edge, 0.0, 0.0), 1.0)
    padded_start = jnp.pad(coarse_start.reshape(NCX, NCY, box_edge), 1)
    parity_fine = parity_of(box_edge, box_edge * box_edge, box_edge)

    def box_anchor(position):
        holder = position // 8
        octant = position % 8
        corner_x = (holder // N_GY) * box_edge + (octant // 4) * half_edge
        corner_y = (holder % N_GY) * box_edge + ((octant // 2) % 2) * half_edge
        corner_z = (octant % 2) * half_edge
        return (corner_x.astype(jnp.int32), corner_y.astype(jnp.int32), corner_z.astype(jnp.int32))

    def smooth_box(operands):
        position, source, coefficient, start = operands
        region = lax.dynamic_slice(padded_start, box_anchor(position), (half_edge + 2, half_edge + 2, half_edge + 2))
        surfaces = [region[0, 1:-1, 1:-1], region[half_edge + 1, 1:-1, 1:-1], region[1:-1, 0, 1:-1], region[1:-1, half_edge + 1, 1:-1], region[1:-1, 1:-1, 0], region[1:-1, 1:-1, half_edge + 1]]
        return fine_sweep(surfaces, source, coefficient, start, first_colour[0], parity_fine, box_edge)

    smoothed, restricted = lax.map(smooth_box, (fine_position, fine_source, fine_coefficient, fine_start))
    resid_volume = resid_c.reshape(NCX, NCY, box_edge)

    def insert(number, volume):
        portion = restricted[number].reshape(half_edge, half_edge, half_edge)
        return lax.dynamic_update_slice(volume, portion, box_anchor(fine_position[number]))

    resid_volume = lax.fori_loop(0, FBOXES, insert, resid_volume)
    composite = resid_volume.reshape(NCX, NCY * box_edge)
    leading = first_colour[1]
    blanks = jnp.zeros_like(composite)
    correction = relaxed(blanks, composite, blanks, diagonal_c, 1.0, parity_coarse, leading)
    coupled = coupling(weights_c, neighbours(correction, outside, box_edge, 0.0, 0.0))
    correction = relaxed(correction, composite, coupled, diagonal_c, 1.0, parity_coarse, 1 - leading)
    leftover = residual_of(correction, composite, weights_c, diagonal_c, neighbours(correction, outside, box_edge, 0.0, 0.0), 1.0)
    bottom_source = coarsen(leftover, box_edge)
    bottom_coefficient = coarsen(coarse_coefficient, box_edge)
    bottom_outside = zero_borders(bottom_source, half_edge)

    def borders_of(values):
        return bottom_outside

    weights_b, diagonal_b = face_terms(bottom_coefficient, neighbours(bottom_coefficient, bottom_outside, half_edge, 0.0, 0.0))
    parity_bottom = parity_of(bottom_source.shape[0], bottom_source.shape[1], half_edge)
    bottom_values = bottom_sweeps(bottom_source, weights_b, diagonal_b, parity_bottom, first_colour[2], borders_of, half_edge)
    correction = correction + refine(bottom_values, half_edge)
    coarse_solution = coarse_start + correction
    correction_volume = correction.reshape(NCX, NCY, box_edge)

    def finish_box(operands):
        position, values = operands
        portion = lax.dynamic_slice(correction_volume, box_anchor(position), (half_edge, half_edge, half_edge))
        return values + refine(portion.reshape(half_edge, half_edge * half_edge), half_edge)

    fine_solution = lax.map(finish_box, (fine_position, smoothed))
    return coarse_solution, fine_solution
```

```python
import functools

import jax
import jax.numpy as jnp
from jax import lax
from jax.experimental import pallas as pl
from jax.experimental.pallas import tpu as pltpu
from jax.sharding import PartitionSpec as P

SWEEPS = 4
LANES = 128
ROWS = 8
F32 = jnp.float32
BF16 = jnp.bfloat16
VMEM = pl.BlockSpec(memory_space=pltpu.VMEM)
SMEM = pl.BlockSpec(memory_space=pltpu.SMEM)


def iotas(shape):
    return (
        lax.broadcasted_iota(jnp.int32, shape, 0),
        lax.broadcasted_iota(jnp.int32, shape, 1),
    )


def ones_where(mask):
    return jnp.where(mask, 1.0, 0.0).astype(BF16)


def select_dot(value, chosen):
    high = value.astype(BF16)
    rest = value - high.astype(F32)
    middle = rest.astype(BF16)
    low = (rest - middle.astype(F32)).astype(BF16)
    total = jnp.dot(low, chosen, preferred_element_type=F32)
    total = total + jnp.dot(middle, chosen, preferred_element_type=F32)
    return total + jnp.dot(high, chosen, preferred_element_type=F32)


def ahead(value, lanes):
    return pltpu.roll(value, value.shape[1] - lanes, 1)


def behind(value, lanes):
    return pltpu.roll(value, lanes, 1)


def parity_block(row, shape, stride):
    x, lane = iotas(shape)
    return (x + row + lane // stride + lane % stride) % 2


def coarsening(edge, fine_lanes, coarse_lanes):
    half = edge // 2
    fine, coarse = iotas((fine_lanes, coarse_lanes))
    same_y = fine // edge // 2 == coarse // half
    return ones_where(same_y & (fine % edge // 2 == coarse % half))


def refining(edge, coarse_lanes, fine_lanes):
    half = edge // 2
    coarse, fine = iotas((coarse_lanes, fine_lanes))
    same_y = fine // edge // 2 == coarse // half
    return ones_where(same_y & (fine % edge // 2 == coarse % half))


def double_rows(ref, value):
    rows = value.shape[0]
    for tile in range(value.shape[1] // LANES):
        part = value[:, tile * LANES : (tile + 1) * LANES]
        ref[tile, pl.ds(0, rows, 2), :] = part
        ref[tile, pl.ds(1, rows, 2), :] = part


def pair_rows(ref, tile, first, rows):
    return ref[tile, pl.ds(first, rows, 2), :] + ref[tile, pl.ds(first + 1, rows, 2), :]


def tiles_of(lane):
    return slice(lane * LANES, (lane + 1) * LANES)


def flat(ref, rows, tiles):
    return jnp.concatenate([ref[tile, rows, :] for tile in tiles], axis=1)


def place(positions, number, groups_y):
    position = positions[number]
    holder = position // 8
    return (holder // groups_y, position % 8)


def residual_kernel(
    groups_x, groups_y, position, start, coefficient, source, low, high,
    residual, upward, downward, slots,
    table,
):
    edge = start.shape[0]
    half = edge // 2
    lanes = start.shape[1]
    unit = LANES
    me = lax.axis_index("gx")
    mine_y = lax.axis_index("gy")
    table[...] = jnp.zeros_like(table)

    wide = lanes + 2 * unit
    _, lane = iotas((ROWS, wide))
    depth = lane % edge
    blank = jnp.zeros((1, wide), F32)
    for row in range(0, edge, ROWS):
        rows = slice(row, row + ROWS)

        def widened(array, offset, rows=rows):
            return jnp.concatenate(
                [
                    low[rows, offset[0] : offset[0] + unit],
                    array[rows, :],
                    high[rows, offset[1] : offset[1] + unit],
                ],
                axis=1,
            )

        v = widened(start, (0, 0))
        k = widened(coefficient, (low.shape[1] - unit, unit))

        def term(k_other, v_other, k=k, v=v):
            return 0.5 * (k + k_other) * (v_other - v)

        total = term(behind(k, edge), behind(v, edge))
        total = total + term(ahead(k, edge), ahead(v, edge))
        first = depth == 0
        last = depth == edge - 1
        total = total + term(
            jnp.where(first, 0.0, behind(k, 1)), jnp.where(first, 0.0, behind(v, 1))
        )
        total = total + term(
            jnp.where(last, 0.0, ahead(k, 1)), jnp.where(last, 0.0, ahead(v, 1))
        )
        total = total[:, unit : unit + lanes]
        v = start[rows, :]
        k = coefficient[rows, :]

        def flux(near, k=k, v=v):
            return 0.5 * (k + coefficient[near, :]) * (start[near, :] - v)

        x, _ = iotas((ROWS, lanes))
        if row == 0:
            near = jnp.concatenate([start[0:1, :], start[0 : ROWS - 1, :]], axis=0)
            knear = jnp.concatenate(
                [coefficient[0:1, :], coefficient[0 : ROWS - 1, :]], axis=0
            )
            total = total + 0.5 * (k + knear) * (near - v)
        else:
            total = total + flux(slice(row - 1, row + ROWS - 1))
        if row + ROWS == edge:
            near = jnp.concatenate(
                [start[row + 1 : edge, :], start[edge - 1 : edge, :]], axis=0
            )
            knear = jnp.concatenate(
                [coefficient[row + 1 : edge, :], coefficient[edge - 1 : edge, :]], axis=0
            )
            total = total + 0.5 * (k + knear) * (near - v)
        else:
            total = total + flux(slice(row + 1, row + ROWS + 1))
        residual[rows, :] = source[rows, :] + total

    pad = low.shape[1] - unit
    for buffer, rows, k_row, v_row in (
        (upward, slice(half, edge), half - 1, edge - 1),
        (downward, slice(0, half), half, 0),
    ):
        buffer[:, 0:lanes] = residual[rows, :]
        buffer[:, lanes : lanes + pad] = low[rows, unit:]
        buffer[:, lanes + pad : 2 * lanes + pad] = coefficient[rows, :]
        body = 2 * lanes + 2 * pad
        buffer[:, 2 * lanes + pad : body] = high[rows, unit:]
        buffer[:, body:] = jnp.zeros((half, buffer.shape[1] - body), F32)
        pieces = []
        for at in range(0, lanes, unit):
            pieces.append((start, v_row, at))
        for at in range(0, pad, unit):
            pieces.append((low, k_row, unit + at))
        for at in range(0, lanes, unit):
            pieces.append((coefficient, k_row, at))
        for at in range(0, pad, unit):
            pieces.append((high, k_row, unit + at))
        for number, (array, row, at) in enumerate(pieces):
            spot = body + number // half * unit
            line = number % half
            buffer[line : line + 1, spot : spot + unit] = array[row : row + 1, at : at + unit]

    span = half * edge
    tiles = span // unit
    unit_y = unit // edge
    wide = span + 2 * unit
    at, to = iotas((wide, unit))
    y = at // edge - unit_y
    z = at % edge
    for octant_x in range(2):
        for octant_y in range(2):
            octant_z = (octant_x + octant_y) % 2
            rows = slice(octant_x * half, octant_x * half + half)
            begin = octant_y * span
            left = (
                low[rows, 0:unit] if octant_y == 0 else start[rows, begin - unit : begin]
            )
            right = (
                start[rows, begin + span : begin + span + unit]
                if octant_y == 0
                else high[rows, 0:unit]
            )
            block = jnp.concatenate([left, start[rows, begin : begin + span], right], axis=1)
            near_z = half if octant_z == 0 else half - 1
            goal = (2 + octant_z) * half
            chosen = (
                ((y == -1) & (to < half) & (z == octant_z * half + to))
                | ((y == half) & (to // half == 1) & (z == octant_z * half + to - half))
                | ((z == near_z) & (to // half == 2 + octant_z) & (y == to - goal))
            )
            entry = 2 * octant_x + octant_y
            table[entry, 0:half, :] = select_dot(block, ones_where(chosen))
            inner = (half, half + ROWS) if octant_x == 0 else (half - ROWS, half)
            outer = (edge - ROWS, edge) if octant_x == 0 else (0, ROWS)
            pick = 0 if octant_x == 0 else ROWS - 1
            outer_pick = ROWS - 1 if octant_x == 0 else 0
            other = 4 + 2 * octant_x + octant_y
            for (first_row, last_row), which, goes, side in (
                (inner, pick, entry, 1 - octant_x),
                (outer, outer_pick, other, octant_x),
            ):
                plane = start[first_row:last_row, begin : begin + span]
                if octant_z == 1:
                    plane = ahead(plane, half)
                for tile in range(tiles):
                    line = half + side * tiles + tile
                    table[goes, line : line + 1, :] = plane[
                        which : which + 1, tile * unit : (tile + 1) * unit
                    ]

    for holder in range(groups_x):
        owner, octant = place(position, holder * groups_y + mine_y, groups_y)
        octant_x = octant // 4
        octant_y = octant // 2 % 2
        entry = jnp.where(
            owner == me,
            2 * octant_x + octant_y,
            jnp.where(owner == me + 1, 4 + octant_y, 6 + octant_y),
        )
        slots[holder] = table[entry]


def fine_kernel(
    groups_x, groups_y, position, colours, faces, source, coefficient, start,
    smoothed, slots,
    ghost, values, kept, rest,
):
    edge = source.shape[0]
    half = edge // 2
    lanes = source.shape[1]
    me = lax.axis_index("gx") * groups_y + lax.axis_index("gy")
    owner, octant = place(position, me, groups_y)
    octant_x = octant // 4
    leading = colours[0]
    span = half * edge
    tiles = span // LANES

    at, to = iotas((LANES, lanes))
    fine_y = to // edge
    fine_z = to % edge
    chosen = (
        ((fine_y == 0) & (at == fine_z // 2))
        | ((fine_y == edge - 1) & (at == half + fine_z // 2))
        | ((fine_z == edge - 1) & (at == 2 * half + fine_y // 2))
        | ((fine_z == 0) & (at == 3 * half + fine_y // 2))
    )
    base = faces[owner]
    sides = select_dot(base[0:half, :], ones_where(chosen))
    double_rows(ghost, sides)
    before = faces[jnp.maximum(owner - 1, 0)][half:, :]
    after = faces[jnp.minimum(owner + 1, groups_x - 1)][half:, :]
    base = base[half:, :]
    before = jnp.where(owner > 0, before, 0.0)
    after = jnp.where(owner < groups_x - 1, after, 0.0)
    line, _ = iotas(base.shape)
    planes = jnp.where(
        line < tiles,
        jnp.where(octant_x == 0, before, base),
        jnp.where(octant_x == 1, after, base),
    )
    unit_fine = 2 * LANES
    at, to = iotas((LANES, unit_fine))
    grown = select_dot(
        planes,
        ones_where((at // edge == to // edge // 2) & (at % edge == to % edge // 2)),
    )
    for tile in range(tiles):
        for part in range(2):
            at = 2 * tile + part
            extra = grown[:, part * LANES : (part + 1) * LANES]
            ghost[at, 0:1, :] = ghost[at, 0:1, :] + extra[tile : tile + 1, :]
            ghost[at, edge - 1 : edge, :] = (
                ghost[at, edge - 1 : edge, :] + extra[tiles + tile : tiles + tile + 1, :]
            )
    every = range(lanes // LANES)

    _, lane = iotas((ROWS, lanes))
    first_y = lane < edge
    last_y = lane >= lanes - edge
    first_z = lane % edge == 0
    last_z = lane % edge == edge - 1

    def weights_at(row):
        k = coefficient[row : row + ROWS, :]
        if row == 0:
            x_low = jnp.concatenate([k[0:1, :], coefficient[0 : ROWS - 1, :]], axis=0)
        else:
            x_low = coefficient[row - 1 : row + ROWS - 1, :]
        if row + ROWS == edge:
            x_high = jnp.concatenate(
                [coefficient[row + 1 : edge, :], k[ROWS - 1 : ROWS, :]], axis=0
            )
        else:
            x_high = coefficient[row + 1 : row + ROWS + 1, :]
        x, _ = iotas((ROWS, lanes))
        outside = (x + row == 0, x + row == edge - 1, first_y, last_y, first_z, last_z)
        around = (x_low, x_high, behind(k, edge), ahead(k, edge), behind(k, 1), ahead(k, 1))
        faces_of = [0.5 * (k + other) for other in around]
        whole = [jnp.where(out, k, w) for out, w in zip(outside, faces_of)]
        diagonal = ((whole[0] + whole[1]) + (whole[2] + whole[3])) + (whole[4] + whole[5])
        inner = [jnp.where(out, 0.0, w) for out, w in zip(outside, faces_of)]
        return k, inner, diagonal

    def around_of(row):
        at = row + ROWS
        v = values[at : at + ROWS, :]
        return (
            values[at - 1 : at + ROWS - 1, :],
            values[at + 1 : at + ROWS + 1, :],
            behind(v, edge),
            ahead(v, edge),
            behind(v, 1),
            ahead(v, 1),
        )

    def summed(weights, around):
        total = weights[0] * around[0]
        for number in range(1, 6):
            total = total + weights[number] * around[number]
        return total

    edges = jnp.zeros((ROWS, lanes), F32)
    values[0:ROWS, :] = edges
    values[edge + ROWS :, :] = edges
    values[ROWS : edge + ROWS, :] = start[...]
    for step in range(2):
        colour = leading if step == 0 else 1 - leading
        fresh_blocks = []
        for row in range(0, edge, ROWS):
            rows = slice(row, row + ROWS)
            k, inner, diagonal = weights_at(row)
            if step == 0:
                kept[rows, :] = source[rows, :] + 4.0 * k * flat(ghost, rows, every)
            fresh = (kept[rows, :] + 4.0 * summed(inner, around_of(row))) / (4.0 * diagonal)
            rest[rows, :] = fresh
        for row in range(0, edge, ROWS):
            rows = slice(row, row + ROWS)
            at = slice(row + ROWS, row + 2 * ROWS)
            parity = parity_block(row, (ROWS, lanes), edge)
            values[at, :] = jnp.where(parity == colour, rest[rows, :], values[at, :])
    for row in range(0, edge, ROWS):
        rows = slice(row, row + ROWS)
        k, inner, diagonal = weights_at(row)
        v = values[row + ROWS : row + 2 * ROWS, :]
        smoothed[rows, :] = v
        value = kept[rows, :] - 4.0 * (diagonal * v - summed(inner, around_of(row)))
        for tile in every:
            ghost[tile, rows, :] = value[:, tiles_of(tile)]
    chosen = coarsening(edge, 4 * LANES, LANES)
    for part in range(lanes // (4 * LANES)):
        block = jnp.concatenate(
            [pair_rows(ghost, 4 * part + tile, 0, half) for tile in range(4)], axis=1
        )
        mean = 0.125 * select_dot(block, chosen)
        for holder in range(groups_x):
            slots[holder, :, part * LANES : (part + 1) * LANES] = mean


def composite_kernel(
    groups_x, groups_y, position, arrived, residual, start, coefficient, below, above,
    composite, upward, downward,
    grown,
):
    edge = start.shape[0]
    half = edge // 2
    lanes = start.shape[1]
    me = lax.axis_index("gx")
    mine_y = lax.axis_index("gy")
    span = half * edge
    composite[0:half, :] = below[:, 0:lanes]
    composite[half : half + edge, :] = residual[...]
    composite[half + edge :, :] = above[:, 0:lanes]
    body = body_lanes(below.shape[1], half)
    k_from = lanes + (body - 2 * lanes) // 2
    for block, mine, theirs, its_row in (
        (below, 0, half - 1, half - 1),
        (above, edge - 1, half + edge, 0),
    ):
        for tile in range(lanes // LANES):
            where = slice(tile * LANES, (tile + 1) * LANES)
            spot = body + tile // half * LANES
            line = tile % half
            v_other = block[line : line + 1, spot : spot + LANES]
            k_other = block[
                its_row : its_row + 1, k_from + tile * LANES : k_from + (tile + 1) * LANES
            ]
            v = start[mine : mine + 1, where]
            flux = 0.5 * (coefficient[mine : mine + 1, where] + k_other) * (v - v_other)
            row = mine + half
            composite[row : row + 1, where] = composite[row : row + 1, where] - flux
            composite[theirs : theirs + 1, where] = composite[theirs : theirs + 1, where] + flux

    at, to = iotas((LANES, 2 * LANES))
    chosen = ones_where((at // half == to // edge) & (at % half == to % half))
    for holder in range(groups_x):
        for part in range(arrived.shape[2] // LANES):
            grown[holder, :, part * 2 * LANES : (part + 1) * 2 * LANES] = select_dot(
                arrived[holder, :, part * LANES : (part + 1) * LANES], chosen
            )
    _, lane = iotas((half, span))
    half_of = lane % edge // half
    for holder in range(groups_x):
        owner, octant = place(position, holder * groups_y + mine_y, groups_y)
        block = 2 * (owner - me) + octant // 4 + 1

        @pl.when((block >= 0) & (block < 4))
        def _(holder=holder, octant=octant, block=block):
            rows = pl.ds(pl.multiple_of(block * half, half), half)
            where = pl.ds(pl.multiple_of(octant // 2 % 2 * span, span), span)
            composite[rows, where] = jnp.where(
                half_of == octant % 2, grown[holder], composite[rows, where]
            )

    upward[...] = composite[:, span:]
    downward[...] = composite[:, 0:span]


def body_lanes(total, rows):
    blocks = total // LANES
    extra = 1
    while -(-(blocks - extra) // rows) != extra:
        extra += 1
    return total - extra * LANES


def coarse_kernel(
    groups_x, groups_y, position, colours, start, coefficient, composite, comp_low,
    comp_high, low, high, below, above,
    solution_ref, slots,
    kext, comp, weights, inverse, first_values, second_values, left, ktiles, bottom, corrected, table,
):
    edge = start.shape[0]
    half = edge // 2
    lanes = start.shape[1]
    span = half * edge
    unit = LANES
    me = lax.axis_index("gx")
    mine_y = lax.axis_index("gy")
    pad = low.shape[1] - unit
    wide = lanes + 2 * pad
    rows_all = 2 * edge
    lanes_all = 2 * lanes
    top = half + ROWS

    kext[top : top + edge, 0:pad] = low[:, unit:]
    kext[top : top + edge, pad : pad + lanes] = coefficient[...]
    kext[top : top + edge, pad + lanes :] = high[:, unit:]
    kext[0:ROWS, :] = jnp.zeros((ROWS, wide), F32)
    kext[top + edge + half :, :] = jnp.zeros((ROWS, wide), F32)
    kext[ROWS:top, :] = below[:, lanes : lanes + wide]
    kext[top + edge : top + edge + half, :] = above[:, lanes : lanes + wide]
    body = lanes + wide
    for tile in range(wide // unit):
        number = lanes // unit + tile
        spot = body + number // half * unit
        line = number % half
        where = slice(tile * unit, (tile + 1) * unit)
        kext[ROWS - 1 : ROWS, where] = below[line : line + 1, spot : spot + unit]
        kext[top + edge + half : top + edge + half + 1, where] = above[
            line : line + 1, spot : spot + unit
        ]
    comp[:, 0:span] = comp_low[...]
    comp[:, span : span + lanes] = composite[...]
    comp[:, span + lanes :] = comp_high[...]

    def inside(shape, row, x_half, x_edge, stride, y_half):
        x, lane = iotas(shape)
        x = x + (row - x_half) + me * x_edge
        y = lane // stride - y_half + mine_y * x_edge
        return (
            (x >= 0) & (x < groups_x * x_edge) & (y >= 0) & (y < groups_y * x_edge)
        )

    def six(k, k_low, k_high, stride, depth_edge):
        _, lane = iotas(k.shape)
        depth = lane % depth_edge
        first = depth == 0
        last = depth == depth_edge - 1
        w = [
            0.5 * (k + k_low),
            0.5 * (k + k_high),
            0.5 * (k + behind(k, stride)),
            0.5 * (k + ahead(k, stride)),
        ]
        z_low = 0.5 * (k + jnp.where(first, 0.0, behind(k, 1)))
        z_high = 0.5 * (k + jnp.where(last, 0.0, ahead(k, 1)))
        diagonal = ((w[0] + w[1]) + (w[2] + w[3])) + (z_low + z_high)
        w = w + [jnp.where(first, 0.0, z_low), jnp.where(last, 0.0, z_high)]
        return w, diagonal

    shift = pad - span
    zero_rows = jnp.zeros((ROWS, lanes_all), F32)
    for ref in (first_values, second_values):
        ref[0:ROWS, :] = zero_rows
        ref[ROWS + rows_all :, :] = zero_rows
    leading = colours[1]
    cut = slice(shift, shift + lanes_all)
    for row in range(0, rows_all, ROWS):
        at = row + ROWS
        k = kext[at : at + ROWS, :]
        w, diagonal = six(
            k, kext[at - 1 : at + ROWS - 1, :], kext[at + 1 : at + ROWS + 1, :], edge, edge
        )
        rows = slice(row, row + ROWS)
        for number in range(6):
            weights[number, rows, :] = w[number][:, cut]
        shape = (ROWS, lanes_all)
        inv = jnp.where(
            inside(shape, row, half, edge, edge, half), 1.0 / diagonal[:, cut], 0.0
        )
        inverse[rows, :] = inv
        parity = parity_block(row, shape, edge)
        first_values[at : at + ROWS, :] = jnp.where(
            parity == leading, comp[rows, :] * inv, 0.0
        )

    def coupled(ref, row):
        at = row + ROWS
        rows = slice(row, row + ROWS)
        v = ref[at : at + ROWS, :]
        total = weights[0, rows, :] * ref[at - 1 : at + ROWS - 1, :]
        total = total + weights[1, rows, :] * ref[at + 1 : at + ROWS + 1, :]
        total = total + weights[2, rows, :] * behind(v, edge)
        total = total + weights[3, rows, :] * ahead(v, edge)
        total = total + weights[4, rows, :] * behind(v, 1)
        return total + weights[5, rows, :] * ahead(v, 1), v

    for row in range(0, rows_all, ROWS):
        rows = slice(row, row + ROWS)
        total, v = coupled(first_values, row)
        parity = parity_block(row, v.shape, edge)
        second_values[row + ROWS : row + 2 * ROWS, :] = jnp.where(
            parity == leading, v, (comp[rows, :] + total) * inverse[rows, :]
        )
    for row in range(0, rows_all, ROWS):
        rows = slice(row, row + ROWS)
        total, v = coupled(second_values, row)
        parity = parity_block(row, v.shape, edge)
        total = jnp.where(parity == leading, total, 0.0)
        for tile in range(lanes_all // unit):
            left[tile, rows, :] = total[:, tiles_of(tile)]
            other = shift // unit + tile
            ktiles[tile, rows, :] = kext[row + ROWS : row + 2 * ROWS, tiles_of(other)]

    chosen = coarsening(edge, 4 * unit, unit)
    bottom_lanes = lanes_all // 4
    f_parts = []
    k_parts = []
    for part in range(bottom_lanes // unit):
        for ref, parts in ((left, f_parts), (ktiles, k_parts)):
            pair = jnp.concatenate(
                [pair_rows(ref, 4 * part + tile, 0, edge) for tile in range(4)], axis=1
            )
            parts.append(0.125 * select_dot(pair, chosen))
    f_bottom = jnp.concatenate(f_parts, axis=1)
    k_bottom = jnp.concatenate(k_parts, axis=1)
    count = edge

    def rows_behind(value):
        return pltpu.roll(value, 1, 0)

    def rows_ahead(value):
        return pltpu.roll(value, count - 1, 0)

    w, diagonal = six(k_bottom, rows_behind(k_bottom), rows_ahead(k_bottom), half, half)
    shape = (edge, bottom_lanes)
    inside_b = inside(shape, 0, half // 2, half, half, half // 2)
    inv = jnp.where(inside_b, 1.0 / (0.25 * diagonal), 0.0)
    w = [0.25 * one for one in w]
    parity = parity_block(0, shape, half)
    values = jnp.zeros(shape, F32)
    for step in range(2 * SWEEPS):
        colour = colours[2] if step % 2 == 0 else 1 - colours[2]
        if step == 0:
            total = f_bottom
        else:
            total = f_bottom + w[0] * rows_behind(values)
            total = total + w[1] * rows_ahead(values)
            total = total + w[2] * behind(values, half)
            total = total + w[3] * ahead(values, half)
            total = total + w[4] * behind(values, 1)
            total = total + w[5] * ahead(values, 1)
        values = jnp.where(parity == colour, total * inv, values)
    bottom[...] = values

    quarter = half // 2
    skip = quarter * half
    chosen = refining(edge, unit, 4 * unit)
    for part in range(lanes // (4 * unit)):
        block = bottom[quarter : quarter + half, skip + part * unit : skip + (part + 1) * unit]
        double_rows(left.at[pl.ds(4 * part, 4)], select_dot(block, chosen))
    for row in range(0, edge, ROWS):
        rows = slice(row, row + ROWS)
        at = row + ROWS + half
        total = flat(left, rows, range(lanes // unit)) + second_values[at : at + ROWS, span : span + lanes]
        corrected[rows, :] = total
        solution_ref[rows, :] = start[rows, :] + total

    at, to = iotas((2 * unit, unit))
    chosen = ones_where((at // edge == to // half) & (at % edge == to % half))
    for octant_x in range(2):
        for octant_y in range(2):
            block = corrected[
                octant_x * half : (octant_x + 1) * half,
                octant_y * span : (octant_y + 1) * span,
            ]
            if (octant_x + octant_y) % 2 == 1:
                block = ahead(block, half)
            for part in range(span // (2 * unit)):
                table[2 * octant_x + octant_y, :, part * unit : (part + 1) * unit] = select_dot(
                    block[:, part * 2 * unit : (part + 1) * 2 * unit], chosen
                )
    for holder in range(groups_x):
        owner, octant = place(position, holder * groups_y + mine_y, groups_y)
        slots[holder] = table[octant // 4 * 2 + octant // 2 % 2]


def finish_kernel(groups_y, position, arrived, smoothed, out, grown):
    edge = smoothed.shape[0]
    half = edge // 2
    me = lax.axis_index("gx") * groups_y + lax.axis_index("gy")
    owner, _ = place(position, me, groups_y)
    value = arrived[owner]
    chosen = refining(edge, LANES, 4 * LANES)
    for part in range(value.shape[1] // LANES):
        fine = select_dot(value[:, tiles_of(part)], chosen)
        double_rows(grown.at[pl.ds(4 * part, 4)], fine)
    out[...] = smoothed[...] + flat(grown, slice(0, edge), range(smoothed.shape[1] // LANES))


def call(kernel, outs, scratch, specs, *operands):
    return pl.pallas_call(
        kernel,
        out_shape=[jax.ShapeDtypeStruct(shape, F32) for shape in outs],
        in_specs=specs,
        out_specs=[VMEM] * len(outs),
        scratch_shapes=[pltpu.VMEM(shape, F32) for shape in scratch],
        compiler_params=pltpu.CompilerParams(vmem_limit_bytes=40 * 1024 * 1024),
    )(*operands)


def tiled(rows, lanes):
    return (lanes // LANES, rows, LANES)


def both_ways(last, first, axis):
    size = lax.axis_size(axis)
    up = [(i, i + 1) for i in range(size - 1)]
    down = [(i + 1, i) for i in range(size - 1)]
    return lax.ppermute(last, axis, up), lax.ppermute(first, axis, down)


def on_device(
    coarse_source,
    coarse_coefficient,
    coarse_start,
    fine_source,
    fine_coefficient,
    fine_start,
    fine_position,
    first_colour,
):
    groups_x = lax.axis_size("gx")
    groups_y = lax.axis_size("gy")
    edge, lanes = coarse_source.shape
    half = edge // 2
    span = half * edge
    pad = span + LANES
    low, high = both_ways(
        jnp.concatenate([coarse_start[:, lanes - LANES :], coarse_coefficient[:, lanes - pad :]], 1),
        jnp.concatenate([coarse_start[:, :LANES], coarse_coefficient[:, :pad]], 1),
        "gy",
    )
    wide = lanes + 2 * pad
    extra = -(-(lanes + wide) // LANES // half) * LANES
    packed = lanes + wide + extra
    face_rows = half + 2 * (span // LANES)
    residual, upward, downward, slots = call(
        functools.partial(residual_kernel, groups_x, groups_y),
        [(edge, lanes), (half, packed), (half, packed), (groups_x, face_rows, LANES)],
        [(8, face_rows, LANES)],
        [SMEM] + [VMEM] * 5,
        fine_position, coarse_start, coarse_coefficient, coarse_source, low, high,
    )
    below, above = both_ways(upward, downward, "gx")
    faces = lax.all_to_all(slots, "gx", 0, 0, tiled=True)
    compact = half * half
    smoothed, restricted = call(
        functools.partial(fine_kernel, groups_x, groups_y),
        [(edge, lanes), (groups_x, half, compact)],
        [tiled(edge, lanes), (edge + 2 * ROWS, lanes), (edge, lanes), (edge, lanes)],
        [SMEM, SMEM] + [VMEM] * 4,
        fine_position, first_colour, faces, fine_source[0], fine_coefficient[0], fine_start[0],
    )
    arrived = lax.all_to_all(restricted, "gx", 0, 0, tiled=True)
    composite, upward, downward = call(
        functools.partial(composite_kernel, groups_x, groups_y),
        [(2 * edge, lanes), (2 * edge, span), (2 * edge, span)],
        [(groups_x, half, span)],
        [SMEM] + [VMEM] * 6,
        fine_position, arrived, residual, coarse_start, coarse_coefficient, below, above,
    )
    comp_low, comp_high = both_ways(upward, downward, "gy")
    rows = 2 * edge
    coarse_solution, slots = call(
        functools.partial(coarse_kernel, groups_x, groups_y),
        [(edge, lanes), (groups_x, half, compact)],
        [
            (rows + 2 * ROWS, wide),
            (rows, 2 * lanes),
            (6, rows, 2 * lanes),
            (rows, 2 * lanes),
            (rows + 2 * ROWS, 2 * lanes),
            (rows + 2 * ROWS, 2 * lanes),
            tiled(rows, 2 * lanes),
            tiled(rows, 2 * lanes),
            (edge, lanes // 2),
            (edge, lanes),
            (4, half, compact),
        ],
        [SMEM, SMEM] + [VMEM] * 9,
        fine_position, first_colour, coarse_start, coarse_coefficient, composite,
        comp_low, comp_high, low, high, below, above,
    )
    returned = lax.all_to_all(slots, "gx", 0, 0, tiled=True)
    (fine_solution,) = call(
        functools.partial(finish_kernel, groups_y),
        [(edge, lanes)],
        [tiled(edge, lanes)],
        [SMEM] + [VMEM] * 2,
        fine_position, returned, smoothed,
    )
    return (coarse_solution, fine_solution[None])


def solution(mesh):
    placed = (
        P("gx", "gy"),
        P("gx", "gy"),
        P("gx", "gy"),
        P(("gx", "gy"), None, None),
        P(("gx", "gy"), None, None),
        P(("gx", "gy"), None, None),
        P(),
        P(),
    )
    return jax.shard_map(
        on_device,
        mesh=mesh,
        in_specs=placed,
        out_specs=(P("gx", "gy"), P(("gx", "gy"), None, None)),
        check_vma=False,
    )
```

```python
import functools

import jax
import jax.numpy as jnp
from jax import lax
from jax.experimental import pallas as pl
from jax.experimental.pallas import tpu as pltpu
from jax.sharding import PartitionSpec as P

SWEEPS = 4
LANES = 128
ROWS = 8
F32 = jnp.float32
BF16 = jnp.bfloat16
VMEM = pl.BlockSpec(memory_space=pltpu.VMEM)
HBM = pl.BlockSpec(memory_space=pl.ANY)


def iotas(shape):
    return (
        lax.broadcasted_iota(jnp.int32, shape, 0),
        lax.broadcasted_iota(jnp.int32, shape, 1),
    )


def ones_where(mask):
    return jnp.where(mask, 1.0, 0.0).astype(BF16)


def select_dot(value, chosen):
    high = value.astype(BF16)
    rest = value - high.astype(F32)
    middle = rest.astype(BF16)
    low = (rest - middle.astype(F32)).astype(BF16)
    rows = value.shape[0]
    if rows % (2 * ROWS) == 0:
        parts = jnp.concatenate([low, middle, high], axis=0)
        whole = jnp.dot(parts, chosen, preferred_element_type=F32)
        return (whole[0:rows] + whole[rows : 2 * rows]) + whole[2 * rows :]
    total = jnp.dot(low, chosen, preferred_element_type=F32)
    total = total + jnp.dot(middle, chosen, preferred_element_type=F32)
    return total + jnp.dot(high, chosen, preferred_element_type=F32)


def ahead(value, lanes):
    return pltpu.roll(value, value.shape[1] - lanes, 1)


def behind(value, lanes):
    return pltpu.roll(value, lanes, 1)


def parity_block(row, shape, stride):
    x, lane = iotas(shape)
    return (x + row + lane // stride + lane % stride) % 2


def coarsening(edge, fine_lanes, coarse_lanes):
    half = edge // 2
    fine, coarse = iotas((fine_lanes, coarse_lanes))
    same_y = fine // edge // 2 == coarse // half
    return ones_where(same_y & (fine % edge // 2 == coarse % half))


def refining(edge, coarse_lanes, fine_lanes):
    half = edge // 2
    coarse, fine = iotas((coarse_lanes, fine_lanes))
    same_y = fine // edge // 2 == coarse // half
    return ones_where(same_y & (fine % edge // 2 == coarse % half))


def double_rows(ref, value):
    rows = value.shape[0]
    for tile in range(value.shape[1] // LANES):
        part = value[:, tile * LANES : (tile + 1) * LANES]
        ref[tile, pl.ds(0, rows, 2), :] = part
        ref[tile, pl.ds(1, rows, 2), :] = part


def pair_rows(ref, tile, first, rows):
    return ref[tile, pl.ds(first, rows, 2), :] + ref[tile, pl.ds(first + 1, rows, 2), :]


def tiles_of(lane):
    return slice(lane * LANES, (lane + 1) * LANES)


def flat(ref, rows, tiles):
    return jnp.concatenate([ref[tile, rows, :] for tile in tiles], axis=1)


def six_faces(k, k_low, k_high, stride, depth_edge):
    _, lane = iotas(k.shape)
    depth = lane % depth_edge
    first = depth == 0
    last = depth == depth_edge - 1
    w = [
        0.5 * (k + k_low),
        0.5 * (k + k_high),
        0.5 * (k + behind(k, stride)),
        0.5 * (k + ahead(k, stride)),
    ]
    z_low = 0.5 * (k + jnp.where(first, 0.0, behind(k, 1)))
    z_high = 0.5 * (k + jnp.where(last, 0.0, ahead(k, 1)))
    diagonal = ((w[0] + w[1]) + (w[2] + w[3])) + (z_low + z_high)
    return w + [jnp.where(first, 0.0, z_low), jnp.where(last, 0.0, z_high)], diagonal


def in_grid(shape, x_first, y_first, stride, x_cells, y_cells):
    x, lane = iotas(shape)
    x = x + x_first
    y = lane // stride + y_first
    return (x >= 0) & (x < x_cells) & (y >= 0) & (y < y_cells)


def two_sides(place_in_axis, size, even, odd):
    parity = place_in_axis % 2
    below = jnp.where(parity == 0, odd, even)
    above = jnp.where(parity == 0, even, odd)
    return (
        jnp.where(place_in_axis > 0, below, 0.0),
        jnp.where(place_in_axis < size - 1, above, 0.0),
    )


def place(positions, number, groups_y):
    _, lane = iotas(positions.shape)
    position = jnp.sum(jnp.where(lane == number, positions[...], 0))
    holder = position // 8
    return (holder // groups_y, position % 8)


def border_kernel(start, coefficient, even_packet, odd_packet, semaphores):
    last = start.shape[1] - LANES
    parity = lax.axis_index("gy") % 2
    copies = []
    for packet, at in (
        (even_packet, (1 - parity) * last),
        (odd_packet, parity * last),
    ):
        for goes, array in enumerate((start, coefficient)):
            copies.append(
                pltpu.make_async_copy(
                    array.at[:, pl.ds(pl.multiple_of(at, LANES), LANES)],
                    packet.at[:, tiles_of(goes)],
                    semaphores.at[len(copies)],
                )
            )
    for copy in copies:
        copy.start()
    for copy in copies:
        copy.wait()


def residual_kernel(
    groups_x, groups_y, position, start, coefficient, source, from_even, from_odd,
    residual, even_packet, odd_packet, slots,
    table, low, high,
):
    edge = start.shape[0]
    half = edge // 2
    lanes = start.shape[1]
    unit = LANES
    me = lax.axis_index("gx")
    mine_y = lax.axis_index("gy")
    table[...] = jnp.zeros_like(table)
    low[...], high[...] = two_sides(mine_y, groups_y, from_even[...], from_odd[...])

    wide = lanes + 2 * unit
    _, lane = iotas((ROWS, wide))
    depth = lane % edge
    blank = jnp.zeros((1, wide), F32)
    for row in range(0, edge, ROWS):
        rows = slice(row, row + ROWS)

        def widened(array, offset, rows=rows):
            return jnp.concatenate(
                [
                    low[rows, offset[0] : offset[0] + unit],
                    array[rows, :],
                    high[rows, offset[1] : offset[1] + unit],
                ],
                axis=1,
            )

        v = widened(start, (0, 0))
        k = widened(coefficient, (unit, unit))

        def term(k_other, v_other, k=k, v=v):
            return 0.5 * (k + k_other) * (v_other - v)

        total = term(behind(k, edge), behind(v, edge))
        total = total + term(ahead(k, edge), ahead(v, edge))
        first = depth == 0
        last = depth == edge - 1
        total = total + term(
            jnp.where(first, 0.0, behind(k, 1)), jnp.where(first, 0.0, behind(v, 1))
        )
        total = total + term(
            jnp.where(last, 0.0, ahead(k, 1)), jnp.where(last, 0.0, ahead(v, 1))
        )
        total = total[:, unit : unit + lanes]
        v = start[rows, :]
        k = coefficient[rows, :]

        def flux(near, k=k, v=v):
            return 0.5 * (k + coefficient[near, :]) * (start[near, :] - v)

        x, _ = iotas((ROWS, lanes))
        if row == 0:
            near = jnp.concatenate([start[0:1, :], start[0 : ROWS - 1, :]], axis=0)
            knear = jnp.concatenate(
                [coefficient[0:1, :], coefficient[0 : ROWS - 1, :]], axis=0
            )
            total = total + 0.5 * (k + knear) * (near - v)
        else:
            total = total + flux(slice(row - 1, row + ROWS - 1))
        if row + ROWS == edge:
            near = jnp.concatenate(
                [start[row + 1 : edge, :], start[edge - 1 : edge, :]], axis=0
            )
            knear = jnp.concatenate(
                [coefficient[row + 1 : edge, :], coefficient[edge - 1 : edge, :]], axis=0
            )
            total = total + 0.5 * (k + knear) * (near - v)
        else:
            total = total + flux(slice(row + 1, row + ROWS + 1))
        residual[rows, :] = source[rows, :] + total

    body = 2 * lanes + 2 * unit

    def pack(buffer, rows, k_row, v_row):
        buffer[:, 0:lanes] = residual[rows, :]
        buffer[:, lanes : lanes + unit] = low[rows, unit:]
        buffer[:, lanes + unit : 2 * lanes + unit] = coefficient[rows, :]
        buffer[:, 2 * lanes + unit : body] = high[rows, unit:]
        buffer[:, body:] = jnp.zeros((half, buffer.shape[1] - body), F32)
        pieces = [(start, v_row, at) for at in range(0, lanes, unit)]
        pieces.append((low, k_row, unit))
        pieces = pieces + [(coefficient, k_row, at) for at in range(0, lanes, unit)]
        pieces.append((high, k_row, unit))
        for number, (array, row, at) in enumerate(pieces):
            spot = body + number // half * unit
            line = number % half
            buffer[line : line + 1, spot : spot + unit] = array[row : row + 1, at : at + unit]

    for parity in range(2):
        upper, lower = (even_packet, odd_packet) if parity == 0 else (odd_packet, even_packet)

        @pl.when(me % 2 == parity)
        def _(upper=upper, lower=lower):
            pack(upper, slice(half, edge), half - 1, edge - 1)
            pack(lower, slice(0, half), half, 0)

    span = half * edge
    tiles = span // unit
    unit_y = unit // edge
    wide = span + 2 * unit
    at, to = iotas((wide, unit))
    y = at // edge - unit_y
    z = at % edge
    for octant_x in range(2):
        for octant_y in range(2):
            octant_z = (octant_x + octant_y) % 2
            rows = slice(octant_x * half, octant_x * half + half)
            begin = octant_y * span
            left = (
                low[rows, 0:unit] if octant_y == 0 else start[rows, begin - unit : begin]
            )
            right = (
                start[rows, begin + span : begin + span + unit]
                if octant_y == 0
                else high[rows, 0:unit]
            )
            block = jnp.concatenate([left, start[rows, begin : begin + span], right], axis=1)
            near_z = half if octant_z == 0 else half - 1
            goal = (2 + octant_z) * half
            chosen = (
                ((y == -1) & (to < half) & (z == octant_z * half + to))
                | ((y == half) & (to // half == 1) & (z == octant_z * half + to - half))
                | ((z == near_z) & (to // half == 2 + octant_z) & (y == to - goal))
            )
            entry = 2 * octant_x + octant_y
            table[entry, 0:half, :] = select_dot(block, ones_where(chosen))
            inner = (half, half + ROWS) if octant_x == 0 else (half - ROWS, half)
            outer = (edge - ROWS, edge) if octant_x == 0 else (0, ROWS)
            pick = 0 if octant_x == 0 else ROWS - 1
            outer_pick = ROWS - 1 if octant_x == 0 else 0
            other = 4 + 2 * octant_x + octant_y
            for (first_row, last_row), which, goes, side in (
                (inner, pick, entry, 1 - octant_x),
                (outer, outer_pick, other, octant_x),
            ):
                plane = start[first_row:last_row, begin : begin + span]
                if octant_z == 1:
                    plane = ahead(plane, half)
                for tile in range(tiles):
                    line = half + side * tiles + tile
                    table[goes, line : line + 1, :] = plane[
                        which : which + 1, tile * unit : (tile + 1) * unit
                    ]

    for holder in range(groups_x):
        owner, octant = place(position, holder * groups_y + mine_y, groups_y)
        octant_x = octant // 4
        octant_y = octant // 2 % 2
        entry = jnp.where(
            owner == me,
            2 * octant_x + octant_y,
            jnp.where(owner == me + 1, 4 + octant_y, 6 + octant_y),
        )
        slots[holder] = table[entry]


def box_terms_kernel(source, coefficient, start, weights, inverse, base):
    edge = source.shape[0]
    lanes = source.shape[1]
    _, lane = iotas((ROWS, lanes))
    first_y = lane < edge
    last_y = lane >= lanes - edge
    first_z = lane % edge == 0
    last_z = lane % edge == edge - 1

    def shifted_rows(array, row):
        block = array[row : row + ROWS, :]
        if row == 0:
            low = jnp.concatenate([block[0:1, :], array[0 : ROWS - 1, :]], axis=0)
        else:
            low = array[row - 1 : row + ROWS - 1, :]
        if row + ROWS == edge:
            high = jnp.concatenate([array[row + 1 : edge, :], block[ROWS - 1 :, :]], axis=0)
        else:
            high = array[row + 1 : row + ROWS + 1, :]
        return (
            block, low, high,
            behind(block, edge), ahead(block, edge), behind(block, 1), ahead(block, 1),
        )

    for row in range(0, edge, ROWS):
        rows = slice(row, row + ROWS)
        x, _ = iotas((ROWS, lanes))
        outside = (x + row == 0, x + row == edge - 1, first_y, last_y, first_z, last_z)
        k, *around = shifted_rows(coefficient, row)
        v, *beside = shifted_rows(start, row)
        total = None
        sums = None
        for number in range(6):
            face = 0.5 * (k + around[number])
            whole = jnp.where(outside[number], k, face)
            inner = jnp.where(outside[number], 0.0, face)
            weights[number, rows, :] = inner
            sums = whole if sums is None else sums + whole
            term = inner * beside[number]
            total = term if total is None else total + term
        inverse[rows, :] = 1.0 / (4.0 * sums)
        base[rows, :] = source[rows, :] + 4.0 * total


def fine_kernel(
    groups_x, groups_y, position, colours, faces, source, coefficient, start,
    weights, inverse, base_terms,
    smoothed, slots,
    ghost, values, kept,
):
    edge = source.shape[0]
    half = edge // 2
    lanes = source.shape[1]
    me = lax.axis_index("gx") * groups_y + lax.axis_index("gy")
    owner, octant = place(position, me, groups_y)
    octant_x = octant // 4
    leading = colours[0:1, 0:1]
    span = half * edge
    tiles = span // LANES

    at, to = iotas((4 * half, lanes))
    fine_y = to // edge
    fine_z = to % edge
    chosen = (
        ((fine_y == 0) & (at == fine_z // 2))
        | ((fine_y == edge - 1) & (at == half + fine_z // 2))
        | ((fine_z == edge - 1) & (at == 2 * half + fine_y // 2))
        | ((fine_z == 0) & (at == 3 * half + fine_y // 2))
    )
    base = faces[owner]
    sides = select_dot(base[0:half, 0 : 4 * half], ones_where(chosen))
    double_rows(ghost, sides)
    before = faces[jnp.maximum(owner - 1, 0)][half:, :]
    after = faces[jnp.minimum(owner + 1, groups_x - 1)][half:, :]
    base = base[half:, :]
    before = jnp.where(owner > 0, before, 0.0)
    after = jnp.where(owner < groups_x - 1, after, 0.0)
    line, _ = iotas(base.shape)
    planes = jnp.where(
        line < tiles,
        jnp.where(octant_x == 0, before, base),
        jnp.where(octant_x == 1, after, base),
    )
    unit_fine = 2 * LANES
    at, to = iotas((LANES, unit_fine))
    grown = select_dot(
        planes,
        ones_where((at // edge == to // edge // 2) & (at % edge == to % edge // 2)),
    )
    for tile in range(tiles):
        for part in range(2):
            at = 2 * tile + part
            extra = grown[:, part * LANES : (part + 1) * LANES]
            ghost[at, 0:1, :] = ghost[at, 0:1, :] + extra[tile : tile + 1, :]
            ghost[at, edge - 1 : edge, :] = (
                ghost[at, edge - 1 : edge, :] + extra[tiles + tile : tiles + tile + 1, :]
            )
    every = range(lanes // LANES)


    edges = jnp.zeros((ROWS, lanes), F32)
    values[0:ROWS, :] = edges
    values[edge + ROWS :, :] = edges
    values[ROWS : edge + ROWS, :] = start[...]

    def coupled(row):
        at = row + ROWS
        rows = slice(row, row + ROWS)
        v = values[at : at + ROWS, :]
        total = weights[0, rows, :] * values[at - 1 : at + ROWS - 1, :]
        total = total + weights[1, rows, :] * values[at + 1 : at + ROWS + 1, :]
        total = total + weights[2, rows, :] * behind(v, edge)
        total = total + weights[3, rows, :] * ahead(v, edge)
        total = total + weights[4, rows, :] * behind(v, 1)
        return total + weights[5, rows, :] * ahead(v, 1), v

    for row in range(0, edge, ROWS):
        rows = slice(row, row + ROWS)
        extra = 4.0 * coefficient[rows, :] * flat(ghost, rows, every)
        parity = parity_block(row, (ROWS, lanes), edge)
        values[row + ROWS : row + 2 * ROWS, :] = jnp.where(
            parity == leading, (base_terms[rows, :] + extra) * inverse[rows, :], start[rows, :]
        )
        kept[rows, :] = source[rows, :] + extra
    for row in range(0, edge, ROWS):
        rows = slice(row, row + ROWS)
        total, v = coupled(row)
        parity = parity_block(row, v.shape, edge)
        smoothed[rows, :] = jnp.where(
            parity == leading, v, (kept[rows, :] + 4.0 * total) * inverse[rows, :]
        )
    values[ROWS : edge + ROWS, :] = smoothed[...]
    for row in range(0, edge, ROWS):
        rows = slice(row, row + ROWS)
        total, v = coupled(row)
        parity = parity_block(row, v.shape, edge)
        value = jnp.where(
            parity == leading, (source[rows, :] - base_terms[rows, :]) + 4.0 * total, 0.0
        )
        for tile in every:
            ghost[tile, rows, :] = value[:, tiles_of(tile)]
    chosen = coarsening(edge, 4 * LANES, LANES)
    for part in range(lanes // (4 * LANES)):
        block = jnp.concatenate(
            [pair_rows(ghost, 4 * part + tile, 0, half) for tile in range(4)], axis=1
        )
        mean = 0.125 * select_dot(block, chosen)
        for holder in range(groups_x):
            slots[holder, :, part * LANES : (part + 1) * LANES] = mean


def coarse_kernel(
    groups_x, groups_y, position, colours, arrived, residual, start, coefficient,
    y_even, y_odd, from_even, from_odd,
    source_b, coefficient_b, correction, even_packet, odd_packet,
    grown, kext, comp, extra_v, weights, inverse, first_values, second_values, left, ktiles,
):
    edge = start.shape[0]
    half = edge // 2
    lanes = start.shape[1]
    span = half * edge
    unit = LANES
    me = lax.axis_index("gx")
    mine_y = lax.axis_index("gy")
    wide = lanes + 2 * unit
    body = lanes + wide
    rows_all = 2 * edge
    top = half + ROWS
    own = slice(unit, unit + lanes)

    k_low, k_high = two_sides(mine_y, groups_y, y_even[:, unit:], y_odd[:, unit:])
    kext[top : top + edge, 0:unit] = k_low
    kext[top : top + edge, own] = coefficient[...]
    kext[top : top + edge, unit + lanes :] = k_high
    kext[0:ROWS, :] = jnp.zeros((ROWS, wide), F32)
    kext[top + edge + half :, :] = jnp.zeros((ROWS, wide), F32)
    comp[:, 0:unit] = jnp.zeros((rows_all, unit), F32)
    comp[:, unit + lanes :] = jnp.zeros((rows_all, unit), F32)
    comp[half : half + edge, own] = residual[...]

    def unpack(block, there, k_rows, c_rows, k_row, number):
        comp[c_rows, own] = jnp.where(there, block[:, 0:lanes], 0.0)
        kext[k_rows, :] = jnp.where(there, block[:, lanes:body], 0.0)
        for piece in range((lanes + wide) // unit):
            spot = body + piece // half * unit
            line = piece % half
            value = jnp.where(there, block[line : line + 1, spot : spot + unit], 0.0)
            if piece < lanes // unit:
                extra_v[number : number + 1, tiles_of(piece)] = value
            else:
                kext[k_row : k_row + 1, tiles_of(piece - lanes // unit)] = value

    for parity in range(2):
        above, below = (from_even, from_odd) if parity == 0 else (from_odd, from_even)

        @pl.when(me % 2 == parity)
        def _(above=above, below=below):
            unpack(below, me > 0, slice(ROWS, top), slice(0, half), ROWS - 1, 0)
            last = top + edge
            unpack(
                above, me < groups_x - 1, slice(last, last + half),
                slice(half + edge, rows_all), last + half, 1,
            )

    for number, mine, theirs in ((0, half, half - 1), (1, half + edge - 1, half + edge)):
        v = start[mine - half : mine - half + 1, :]
        k = kext[mine + ROWS : mine + ROWS + 1, own]
        k_other = kext[theirs + ROWS : theirs + ROWS + 1, own]
        flux = 0.5 * (k + k_other) * (v - extra_v[number : number + 1, :])
        comp[mine : mine + 1, own] = comp[mine : mine + 1, own] - flux
        comp[theirs : theirs + 1, own] = comp[theirs : theirs + 1, own] + flux

    at, to = iotas((unit, 2 * unit))
    chosen = ones_where((at // half == to // edge) & (at % half == to % half))
    for part in range(arrived.shape[2] // unit):
        every = arrived[:, :, tiles_of(part)].reshape(groups_x * half, unit)
        grown[:, part * 2 * unit : (part + 1) * 2 * unit] = select_dot(every, chosen)
    _, lane = iotas((half, span))
    half_of = lane % edge // half
    for holder in range(groups_x):
        owner, octant = place(position, holder * groups_y + mine_y, groups_y)
        block = 2 * (owner - me) + octant // 4 + 1

        @pl.when((block >= 0) & (block < 4))
        def _(holder=holder, octant=octant, block=block):
            rows = pl.ds(pl.multiple_of(block * half, half), half)
            where = pl.ds(pl.multiple_of(unit + octant // 2 % 2 * span, unit), span)
            comp[rows, where] = jnp.where(
                half_of == octant % 2,
                grown[holder * half : (holder + 1) * half, :],
                comp[rows, where],
            )

    zero_rows = jnp.zeros((ROWS, wide), F32)
    for ref in (first_values, second_values):
        ref[0:ROWS, :] = zero_rows
        ref[ROWS + rows_all :, :] = zero_rows
    leading = colours[0:1, 1:2]
    shape = (ROWS, wide)
    for row in range(0, rows_all, ROWS):
        at = row + ROWS
        rows = slice(row, row + ROWS)
        w, diagonal = six_faces(
            kext[at : at + ROWS, :],
            kext[at - 1 : at + ROWS - 1, :],
            kext[at + 1 : at + ROWS + 1, :],
            edge,
            edge,
        )
        for number in range(6):
            weights[number, rows, :] = w[number]
        inside = in_grid(
            shape, row - half + me * edge, mine_y * edge - unit // edge, edge,
            groups_x * edge, groups_y * edge,
        )
        inv = jnp.where(inside, 1.0 / diagonal, 0.0)
        inverse[rows, :] = inv
        parity = parity_block(row, shape, edge)
        first_values[at : at + ROWS, :] = jnp.where(
            parity == leading, comp[rows, :] * inv, 0.0
        )

    def coupled(ref, row):
        at = row + ROWS
        rows = slice(row, row + ROWS)
        v = ref[at : at + ROWS, :]
        total = weights[0, rows, :] * ref[at - 1 : at + ROWS - 1, :]
        total = total + weights[1, rows, :] * ref[at + 1 : at + ROWS + 1, :]
        total = total + weights[2, rows, :] * behind(v, edge)
        total = total + weights[3, rows, :] * ahead(v, edge)
        total = total + weights[4, rows, :] * behind(v, 1)
        return total + weights[5, rows, :] * ahead(v, 1), v

    for row in range(0, rows_all, ROWS):
        rows = slice(row, row + ROWS)
        total, v = coupled(first_values, row)
        parity = parity_block(row, v.shape, edge)
        second_values[row + ROWS : row + 2 * ROWS, :] = jnp.where(
            parity == leading, v, (comp[rows, :] + total) * inverse[rows, :]
        )
    for row in range(0, rows_all, ROWS):
        rows = slice(row, row + ROWS)
        total, v = coupled(second_values, row)
        parity = parity_block(row, v.shape, edge)
        total = jnp.where(parity == leading, total, 0.0)
        for tile in range(wide // unit):
            left[tile, rows, :] = total[:, tiles_of(tile)]
        for tile in range(lanes // unit):
            ktiles[tile, rows, :] = kext[row + ROWS : row + 2 * ROWS, tiles_of(tile + 1)]

    chosen = coarsening(edge, 4 * unit, unit)

    def pairs(ref, tiles):
        return jnp.concatenate([pair_rows(ref, tile, 0, edge) for tile in tiles], axis=1)

    blocks = lanes // unit // 4
    last = wide // unit - 1
    source_b[:, 0:unit] = 0.125 * select_dot(pairs(left, [0]), chosen[3 * unit :, :])
    source_b[:, (blocks + 1) * unit :] = 0.125 * select_dot(
        pairs(left, [last]), chosen[0:unit, :]
    )
    for part in range(blocks):
        source_b[:, tiles_of(part + 1)] = 0.125 * select_dot(
            pairs(left, range(4 * part + 1, 4 * part + 5)), chosen
        )
        coefficient_b[:, tiles_of(part)] = 0.125 * select_dot(
            pairs(ktiles, range(4 * part, 4 * part + 4)), chosen
        )
    middle = (blocks + 2) // 2 * unit
    rows = slice(ROWS + half, ROWS + half + edge)
    correction[...] = second_values[rows, own]
    for parity in range(2):
        up, down = (even_packet, odd_packet) if parity == 0 else (odd_packet, even_packet)

        @pl.when(mine_y % 2 == parity)
        def _(up=up, down=down):
            up[:, 0:middle] = source_b[:, middle:]
            up[:, middle : middle + unit] = coefficient_b[:, (blocks - 1) * unit :]
            up[:, middle + unit :] = second_values[rows, unit + lanes :]
            down[:, 0:middle] = source_b[:, 0:middle]
            down[:, middle : middle + unit] = coefficient_b[:, 0:unit]
            down[:, middle + unit :] = second_values[rows, 0:unit]


def bottom_kernel(
    groups_x, groups_y, position, colours, source_b, coefficient_b, correction,
    from_even, from_odd,
    corrected, slots,
    bottom, spread, table, low, high,
):
    edge = correction.shape[0]
    half = edge // 2
    lanes = correction.shape[1]
    span = half * edge
    unit = LANES
    me = lax.axis_index("gx")
    mine_y = lax.axis_index("gy")
    low[...], high[...] = two_sides(mine_y, groups_y, from_even[...], from_odd[...])
    shape = source_b.shape
    middle = shape[1] // 2
    f_bottom = source_b[...] + jnp.concatenate([low[:, 0:middle], high[:, 0:middle]], axis=1)
    k_bottom = jnp.concatenate(
        [
            low[:, middle : middle + unit],
            coefficient_b[...],
            high[:, middle : middle + unit],
        ],
        axis=1,
    )
    quarter = half // 2

    def rows_behind(value):
        return pltpu.roll(value, 1, 0)

    def rows_ahead(value):
        return pltpu.roll(value, edge - 1, 0)

    w, diagonal = six_faces(k_bottom, rows_behind(k_bottom), rows_ahead(k_bottom), half, half)
    inside = in_grid(
        shape, me * half - quarter, mine_y * half - unit // half, half,
        groups_x * half, groups_y * half,
    )
    inv = jnp.where(inside, 1.0 / (0.25 * diagonal), 0.0)
    w = [0.25 * one for one in w]
    parity = parity_block(0, shape, half)
    values = jnp.zeros(shape, F32)
    first = colours[0:1, 2:3]
    for step in range(2 * SWEEPS):
        colour = first if step % 2 == 0 else 1 - first
        if step == 0:
            total = f_bottom
        else:
            total = f_bottom + w[0] * rows_behind(values)
            total = total + w[1] * rows_ahead(values)
            total = total + w[2] * behind(values, half)
            total = total + w[3] * ahead(values, half)
            total = total + w[4] * behind(values, 1)
            total = total + w[5] * ahead(values, 1)
        values = jnp.where(parity == colour, total * inv, values)
    bottom[...] = values

    chosen = refining(edge, unit, 4 * unit)
    for part in range(lanes // (4 * unit)):
        block = bottom[quarter : quarter + half, tiles_of(part + 1)]
        double_rows(spread.at[pl.ds(4 * part, 4)], select_dot(block, chosen))
    every = range(lanes // unit)
    for row in range(0, edge, ROWS):
        rows = slice(row, row + ROWS)
        total = correction[rows, :] + flat(spread, rows, every)
        ring = [total[:, tiles_of(tile)] for tile in every]
        ring[0] = ring[0] + low[rows, middle + unit :]
        ring[-1] = ring[-1] + high[rows, middle + unit :]
        total = jnp.concatenate(ring, axis=1)
        corrected[rows, :] = total

    at, to = iotas((2 * unit, unit))
    chosen = ones_where((at // edge == to // half) & (at % edge == to % half))
    for octant_x in range(2):
        for octant_y in range(2):
            block = corrected[
                octant_x * half : (octant_x + 1) * half,
                octant_y * span : (octant_y + 1) * span,
            ]
            if (octant_x + octant_y) % 2 == 1:
                block = ahead(block, half)
            for part in range(span // (2 * unit)):
                table[2 * octant_x + octant_y, :, part * unit : (part + 1) * unit] = select_dot(
                    block[:, part * 2 * unit : (part + 1) * 2 * unit], chosen
                )
    for holder in range(groups_x):
        owner, octant = place(position, holder * groups_y + mine_y, groups_y)
        slots[holder] = table[octant // 4 * 2 + octant // 2 % 2]


def finish_kernel(
    groups_y, position, arrived, smoothed, start, correction, coarse_out, out, grown
):
    edge = smoothed.shape[0]
    half = edge // 2
    me = lax.axis_index("gx") * groups_y + lax.axis_index("gy")
    owner, _ = place(position, me, groups_y)
    coarse_out[...] = start[...] + correction[...]
    value = arrived[owner]
    chosen = refining(edge, LANES, 4 * LANES)
    for part in range(value.shape[1] // LANES):
        fine = select_dot(value[:, tiles_of(part)], chosen)
        double_rows(grown.at[pl.ds(4 * part, 4)], fine)
    out[...] = smoothed[...] + flat(grown, slice(0, edge), range(smoothed.shape[1] // LANES))


def call(kernel, outs, scratch, specs, *operands):
    return pl.pallas_call(
        kernel,
        out_shape=[jax.ShapeDtypeStruct(shape, F32) for shape in outs],
        in_specs=specs,
        out_specs=[VMEM] * len(outs),
        scratch_shapes=[pltpu.VMEM(shape, F32) for shape in scratch],
        compiler_params=pltpu.CompilerParams(vmem_limit_bytes=40 * 1024 * 1024),
    )(*operands)


def tiled(rows, lanes):
    return (lanes // LANES, rows, LANES)


def matching(axis, first):
    sizes = (lax.axis_size("gx"), lax.axis_size("gy"))
    along_x = axis == "gx"
    size, others = sizes if along_x else sizes[::-1]
    pairs = []
    for other in range(others):
        for i in range(size):
            j = i + 1 if (i - first) % 2 == 0 else i - 1
            goes, beside = j, other
            if not 0 <= j < size:
                goes, beside = i, other ^ 1
            if beside < others:
                here, there = (i, other), (goes, beside)
                if not along_x:
                    here, there = here[::-1], there[::-1]
                pairs.append((here[0] * sizes[1] + here[1], there[0] * sizes[1] + there[1]))
    return pairs


def swapped(even_packet, odd_packet, axis):
    return tuple(
        lax.ppermute(packet, ("gx", "gy"), matching(axis, first))
        for first, packet in ((0, even_packet), (1, odd_packet))
    )


def on_device(
    coarse_source,
    coarse_coefficient,
    coarse_start,
    fine_source,
    fine_coefficient,
    fine_start,
    fine_position,
    first_colour,
):
    groups_x = lax.axis_size("gx")
    groups_y = lax.axis_size("gy")
    edge, lanes = coarse_source.shape
    half = edge // 2
    span = half * edge
    compact = half * half
    wide = lanes + 2 * LANES
    positions = fine_position.reshape(1, -1)
    colours = first_colour.reshape(1, -1)
    packets = pl.pallas_call(
        border_kernel,
        out_shape=[jax.ShapeDtypeStruct((edge, 2 * LANES), F32)] * 2,
        in_specs=[HBM] * 2,
        out_specs=[VMEM] * 2,
        scratch_shapes=[pltpu.SemaphoreType.DMA((4,))],
    )(coarse_start, coarse_coefficient)
    y_even, y_odd = swapped(*packets, "gy")
    box = (fine_source[0], fine_coefficient[0], fine_start[0])
    weights, inverse, base = call(
        box_terms_kernel, [(6, edge, lanes), (edge, lanes), (edge, lanes)], [], [VMEM] * 3, *box
    )
    extra = -(-(lanes + wide) // LANES // half) * LANES
    packed = lanes + wide + extra
    face_rows = half + 2 * (span // LANES)
    residual, even_packet, odd_packet, slots = call(
        functools.partial(residual_kernel, groups_x, groups_y),
        [(edge, lanes), (half, packed), (half, packed), (groups_x, face_rows, LANES)],
        [(8, face_rows, LANES), (edge, 2 * LANES), (edge, 2 * LANES)],
        [VMEM] * 6,
        positions, coarse_start, coarse_coefficient, coarse_source, y_even, y_odd,
    )
    from_even, from_odd = swapped(even_packet, odd_packet, "gx")
    faces = lax.all_to_all(slots, "gx", 0, 0, tiled=True)
    smoothed, restricted = call(
        functools.partial(fine_kernel, groups_x, groups_y),
        [(edge, lanes), (groups_x, half, compact)],
        [tiled(edge, lanes), (edge + 2 * ROWS, lanes), (edge, lanes)],
        [VMEM] * 9,
        positions, colours, faces, *box, weights, inverse, base,
    )
    arrived = lax.all_to_all(restricted, "gx", 0, 0, tiled=True)
    rows = 2 * edge
    lanes_b = (wide // LANES - 2) // 4 * LANES
    source_b, coefficient_b, correction, even_packet, odd_packet = call(
        functools.partial(coarse_kernel, groups_x, groups_y),
        [
            (edge, lanes_b + 2 * LANES),
            (edge, lanes_b),
            (edge, lanes),
            (edge, lanes_b // 2 + 3 * LANES),
            (edge, lanes_b // 2 + 3 * LANES),
        ],
        [
            (groups_x * half, span),
            (rows + 2 * ROWS, wide),
            (rows, wide),
            (ROWS, lanes),
            (6, rows, wide),
            (rows, wide),
            (rows + 2 * ROWS, wide),
            (rows + 2 * ROWS, wide),
            tiled(rows, wide),
            tiled(rows, lanes),
        ],
        [VMEM] * 10,
        positions, colours, arrived, residual, coarse_start, coarse_coefficient,
        y_even, y_odd, from_even, from_odd,
    )
    y_even, y_odd = swapped(even_packet, odd_packet, "gy")
    corrected, slots = call(
        functools.partial(bottom_kernel, groups_x, groups_y),
        [(edge, lanes), (groups_x, half, compact)],
        [(edge, lanes_b + 2 * LANES), tiled(edge, lanes), (4, half, compact)]
        + [(edge, lanes_b // 2 + 3 * LANES)] * 2,
        [VMEM] * 7,
        positions, colours, source_b, coefficient_b, correction, y_even, y_odd,
    )
    returned = lax.all_to_all(slots, "gx", 0, 0, tiled=True)
    coarse_solution, fine_solution = call(
        functools.partial(finish_kernel, groups_y),
        [(edge, lanes), (edge, lanes)],
        [tiled(edge, lanes)],
        [VMEM] * 5,
        positions, returned, smoothed, coarse_start, corrected,
    )
    return (coarse_solution, fine_solution[None])


def solution(mesh):
    placed = (
        P("gx", "gy"),
        P("gx", "gy"),
        P("gx", "gy"),
        P(("gx", "gy"), None, None),
        P(("gx", "gy"), None, None),
        P(("gx", "gy"), None, None),
        P(),
        P(),
    )
    return jax.shard_map(
        on_device,
        mesh=mesh,
        in_specs=placed,
        out_specs=(P("gx", "gy"), P(("gx", "gy"), None, None)),
        check_vma=False,
    )
```

```python
import functools

import jax
import jax.numpy as jnp
from jax import lax
from jax.experimental import pallas as pl
from jax.experimental.pallas import tpu as pltpu
from jax.sharding import PartitionSpec as P


SWEEPS = 4
LANES = 128
ROWS = 8
F32 = jnp.float32
BF16 = jnp.bfloat16
VMEM = pl.BlockSpec(memory_space=pltpu.VMEM)
HBM = pl.BlockSpec(memory_space=pltpu.HBM)
PARAMS = pltpu.CompilerParams(vmem_limit_bytes=20 * 1024 * 1024)


def iotas(shape):
    return (
        lax.broadcasted_iota(jnp.int32, shape, 0),
        lax.broadcasted_iota(jnp.int32, shape, 1),
    )


def ones_where(mask):
    return jnp.where(mask, 1.0, 0.0).astype(BF16)


def select_dot(value, chosen):
    high = value.astype(BF16)
    rest = value - high.astype(F32)
    middle = rest.astype(BF16)
    low = (rest - middle.astype(F32)).astype(BF16)
    rows = value.shape[0]
    if rows % (2 * ROWS) == 0:
        parts = jnp.concatenate([low, middle, high], axis=0)
        whole = jnp.dot(parts, chosen, preferred_element_type=F32)
        return (whole[0:rows] + whole[rows : 2 * rows]) + whole[2 * rows :]
    total = jnp.dot(low, chosen, preferred_element_type=F32)
    total = total + jnp.dot(middle, chosen, preferred_element_type=F32)
    return total + jnp.dot(high, chosen, preferred_element_type=F32)


def ahead(value, lanes):
    return pltpu.roll(value, value.shape[1] - lanes, 1)


def behind(value, lanes):
    return pltpu.roll(value, lanes, 1)


def cell_parity(edge):
    x, lane = iotas((ROWS, LANES))
    return (x + lane // edge + lane % edge) % 2


def along_y(tiles, edge):
    _, lane = iotas(tiles[0].shape)
    up = [0.0] + [pltpu.roll(one, edge, 1) for one in tiles]
    down = [pltpu.roll(one, LANES - edge, 1) for one in tiles] + [0.0]
    count = len(tiles)
    low = [jnp.where(lane < edge, up[t], up[t + 1]) for t in range(count)]
    high = [jnp.where(lane >= LANES - edge, down[t + 1], down[t]) for t in range(count)]
    return low, high


def along_z(tiles):
    return (
        [pltpu.roll(one, 1, 1) for one in tiles],
        [pltpu.roll(one, LANES - 1, 1) for one in tiles],
    )


def six_around(ref, tiles, at, edge):
    own = [ref[t, at : at + ROWS, :] for t in tiles]
    x_low = [ref[t, at - 1 : at + ROWS - 1, :] for t in tiles]
    x_high = [ref[t, at + 1 : at + ROWS + 1, :] for t in tiles]
    return own, (x_low, x_high) + along_y(own, edge) + along_z(own)


def coupled(weights, rows, ref, tiles, at, edge):
    own, around = six_around(ref, tiles, at, edge)
    sums = []
    for spot, tile in enumerate(tiles):
        total = weights[0, tile, rows, :] * around[0][spot]
        for number in range(1, 6):
            total = total + weights[number, tile, rows, :] * around[number][spot]
        sums.append(total)
    return own, sums


def coarsening(edge, fine_lanes, coarse_lanes):
    half = edge // 2
    fine, coarse = iotas((fine_lanes, coarse_lanes))
    same_y = fine // edge // 2 == coarse // half
    return ones_where(same_y & (fine % edge // 2 == coarse % half))


def refining(edge, coarse_lanes, fine_lanes):
    half = edge // 2
    coarse, fine = iotas((coarse_lanes, fine_lanes))
    same_y = fine // edge // 2 == coarse // half
    return ones_where(same_y & (fine % edge // 2 == coarse % half))


def double_rows(ref, value):
    rows = value.shape[0]
    for tile in range(value.shape[1] // LANES):
        part = value[:, tile * LANES : (tile + 1) * LANES]
        ref[tile, pl.ds(0, rows, 2), :] = part
        ref[tile, pl.ds(1, rows, 2), :] = part


def pair_rows(ref, tile, first, rows):
    return ref[tile, pl.ds(first, rows, 2), :] + ref[tile, pl.ds(first + 1, rows, 2), :]


def tiles_of(lane):
    return slice(lane * LANES, (lane + 1) * LANES)


def flat(ref, rows, tiles):
    return jnp.concatenate([ref[tile, rows, :] for tile in tiles], axis=1)


def twice_faces(own, around, edge):
    _, lane = iotas(own[0].shape)
    first = lane % edge == 0
    last = lane % edge == edge - 1
    weights = []
    diagonals = []
    for spot, k in enumerate(own):
        w = [k + around[number][spot] for number in range(6)]
        diagonals.append(
            ((w[0] + w[1]) + (w[2] + w[3]))
            + (jnp.where(first, k, w[4]) + jnp.where(last, k, w[5]))
        )
        w[4] = jnp.where(first, 0.0, w[4])
        w[5] = jnp.where(last, 0.0, w[5])
        weights.append(w)
    return weights, diagonals


def two_sides(place_in_axis, size, even, odd):
    parity = place_in_axis % 2
    below = jnp.where(parity == 0, odd, even)
    above = jnp.where(parity == 0, even, odd)
    return (
        jnp.where(place_in_axis > 0, below, 0.0),
        jnp.where(place_in_axis < size - 1, above, 0.0),
    )


def place(positions, number, groups_y):
    _, lane = iotas(positions.shape)
    position = jnp.sum(jnp.where(lane == number, positions[...], 0))
    holder = position // 8
    return (holder // groups_y, position % 8)


def select_faces(edge, octant_z):
    half = edge // 2
    unit_y = LANES // edge
    at, to = iotas((half * edge + 2 * LANES, LANES))
    y = at // edge - unit_y
    z = at % edge
    near_z = half if octant_z == 0 else half - 1
    goal = (2 + octant_z) * half
    which = to // half
    spot = to % half
    return ones_where(
        ((y == -1) & (which == 0) & (z == octant_z * half + spot))
        | ((y == half) & (which == 1) & (z == octant_z * half + spot))
        | ((z == near_z) & (which == 2 + octant_z) & (y == to - goal))
    )


def select_ghosts(edge, lanes):
    half = edge // 2
    at, to = iotas((4 * half, lanes))
    fine_y = to // edge
    fine_z = to % edge
    return ones_where(
        ((fine_y == 0) & (at == fine_z // 2))
        | ((fine_y == edge - 1) & (at == half + fine_z // 2))
        | ((fine_z == edge - 1) & (at == 2 * half + fine_y // 2))
        | ((fine_z == 0) & (at == 3 * half + fine_y // 2))
    )


def select_planes(edge):
    at, to = iotas((LANES, 2 * LANES))
    return ones_where((at // edge == to // edge // 2) & (at % edge == to % edge // 2))


def select_both_halves(edge):
    half = edge // 2
    at, to = iotas((LANES, 2 * LANES))
    return ones_where((at // half == to // edge) & (at % half == to % half))


def select_low_half(edge):
    half = edge // 2
    at, to = iotas((2 * LANES, LANES))
    return ones_where((at // edge == to // half) & (at % edge == to % half))


def border_kernel(
    start, coefficient, position, colours,
    even_packet, odd_packet, position_out, colours_out, faces_0, faces_1,
    semaphores,
):
    edge, lanes = start.shape
    last = lanes - LANES
    parity = lax.axis_index("gy") % 2
    copies = []
    for packet, at in (
        (even_packet, (1 - parity) * last),
        (odd_packet, parity * last),
    ):
        for goes, array in enumerate((start, coefficient)):
            copies.append(
                pltpu.make_async_copy(
                    array.at[:, pl.ds(pl.multiple_of(at, LANES), LANES)],
                    packet.at[:, tiles_of(goes)],
                    semaphores.at[len(copies)],
                )
            )
    for array, goes in ((position, position_out), (colours, colours_out)):
        copies.append(pltpu.make_async_copy(array, goes, semaphores.at[len(copies)]))
    for copy in copies:
        copy.start()
    faces_0[...] = select_faces(edge, 0)
    faces_1[...] = select_faces(edge, 1)
    for copy in copies:
        copy.wait()


def faces_kernel(
    groups_x, groups_y, position, colours, start, from_even, from_odd, faces_0, faces_1,
    slots,
    table, low, high,
):
    edge = start.shape[0]
    half = edge // 2
    unit = LANES
    me = lax.axis_index("gx")
    mine_y = lax.axis_index("gy")
    table[...] = jnp.zeros_like(table)
    low[...], high[...] = two_sides(
        mine_y, groups_y, from_even[:, 0:unit], from_odd[:, 0:unit]
    )

    span = half * edge
    tiles = span // unit
    chosen = (faces_0[...], faces_1[...])
    for octant_x in range(2):
        for octant_y in range(2):
            octant_z = (octant_x + octant_y) % 2
            rows = slice(octant_x * half, octant_x * half + half)
            begin = octant_y * span
            left = (
                low[rows, 0:unit] if octant_y == 0 else start[rows, begin - unit : begin]
            )
            right = (
                start[rows, begin + span : begin + span + unit]
                if octant_y == 0
                else high[rows, 0:unit]
            )
            block = jnp.concatenate([left, start[rows, begin : begin + span], right], axis=1)
            entry = 2 * octant_x + octant_y
            table[entry, 0:half, :] = select_dot(block, chosen[octant_z])
            inner = (half, half + ROWS) if octant_x == 0 else (half - ROWS, half)
            outer = (edge - ROWS, edge) if octant_x == 0 else (0, ROWS)
            pick = 0 if octant_x == 0 else ROWS - 1
            outer_pick = ROWS - 1 if octant_x == 0 else 0
            other = 4 + 2 * octant_x + octant_y
            for (first_row, last_row), which, goes, side in (
                (inner, pick, entry, 1 - octant_x),
                (outer, outer_pick, other, octant_x),
            ):
                plane = start[first_row:last_row, begin : begin + span]
                if octant_z == 1:
                    plane = ahead(plane, half)
                for tile in range(tiles):
                    line = half + side * tiles + tile
                    table[goes, line : line + 1, :] = plane[
                        which : which + 1, tile * unit : (tile + 1) * unit
                    ]

    for holder in range(groups_x):
        owner, octant = place(position, holder * groups_y + mine_y, groups_y)
        octant_x = octant // 4
        octant_y = octant // 2 % 2
        entry = jnp.where(
            owner == me,
            2 * octant_x + octant_y,
            jnp.where(owner == me + 1, 4 + octant_y, 6 + octant_y),
        )
        slots[holder] = table[entry]


def residual_kernel(
    groups_y, start, coefficient, source, from_even, from_odd,
    residual, even_packet, odd_packet,
    values, kappas, low, high,
):
    edge = start.shape[0]
    half = edge // 2
    lanes = start.shape[1]
    unit = LANES
    me = lax.axis_index("gx")
    mine_y = lax.axis_index("gy")
    low[...], high[...] = two_sides(mine_y, groups_y, from_even[...], from_odd[...])
    every = range(lanes // unit)
    for ref, array, border in ((values, start, 0), (kappas, coefficient, 1)):
        ref[0, ROWS : ROWS + edge, :] = low[:, tiles_of(border)]
        ref[lanes // unit + 1, ROWS : ROWS + edge, :] = high[:, tiles_of(border)]
        for tile in every:
            ref[tile + 1, ROWS - 1 : ROWS, :] = array[0:1, tiles_of(tile)]
            ref[tile + 1, ROWS : ROWS + edge, :] = array[:, tiles_of(tile)]
            ref[tile + 1, ROWS + edge : ROWS + edge + 1, :] = array[edge - 1 :, tiles_of(tile)]
    _, lane = iotas((ROWS, unit))
    first = lane % edge == 0
    last = lane % edge == edge - 1
    for row in range(0, edge, ROWS):
        at = row + ROWS
        for tile in every:
            near = (tile, tile + 1, tile + 2)
            v = values[tile + 1, at : at + ROWS, :]
            k = kappas[tile + 1, at : at + ROWS, :]
            total = 2.0 * source[row : row + ROWS, tiles_of(tile)]
            for move in (-1, 1):
                rows = slice(at + move, at + move + ROWS)
                total = total + (k + kappas[tile + 1, rows, :]) * (values[tile + 1, rows, :] - v)
            vs = along_y([values[t, at : at + ROWS, :] for t in near], edge)
            ks = along_y([kappas[t, at : at + ROWS, :] for t in near], edge)
            for side in range(2):
                total = total + (k + ks[side][1]) * (vs[side][1] - v)
            vz = along_z([v])
            kz = along_z([k])
            for side, border in ((0, first), (1, last)):
                k_other = jnp.where(border, 0.0, kz[side][0])
                v_other = jnp.where(border, 0.0, vz[side][0])
                total = total + (k + k_other) * (v_other - v)
            residual[tile, row : row + ROWS, :] = total

    body = 2 * lanes + 2 * unit

    def pack(buffer, rows, k_row, v_row):
        for tile in every:
            buffer[:, tiles_of(tile)] = residual[tile, rows, :]
        buffer[:, lanes : lanes + unit] = low[rows, unit:]
        buffer[:, lanes + unit : 2 * lanes + unit] = coefficient[rows, :]
        buffer[:, 2 * lanes + unit : body] = high[rows, unit:]
        buffer[:, body:] = jnp.zeros((half, buffer.shape[1] - body), F32)
        pieces = [(start, v_row, at) for at in range(0, lanes, unit)]
        pieces.append((low, k_row, unit))
        pieces = pieces + [(coefficient, k_row, at) for at in range(0, lanes, unit)]
        pieces.append((high, k_row, unit))
        for number, (array, row, at) in enumerate(pieces):
            spot = body + number // half * unit
            line = number % half
            buffer[line : line + 1, spot : spot + unit] = array[row : row + 1, at : at + unit]

    for parity in range(2):
        upper, lower = (even_packet, odd_packet) if parity == 0 else (odd_packet, even_packet)

        @pl.when(me % 2 == parity)
        def _(upper=upper, lower=lower):
            pack(upper, slice(half, edge), half - 1, edge - 1)
            pack(lower, slice(0, half), half, 0)


def box_terms_kernel(
    source, coefficient, start,
    weights, inverse, base, ghosts, planes, both, low_half, coarsen, refine,
):
    edge = source.shape[0]
    lanes = source.shape[1]
    _, lane = iotas((ROWS, lanes))
    first_y = lane < edge
    last_y = lane >= lanes - edge
    first_z = lane % edge == 0
    last_z = lane % edge == edge - 1

    def shifted_rows(array, row):
        block = array[row : row + ROWS, :]
        if row == 0:
            low = jnp.concatenate([block[0:1, :], array[0 : ROWS - 1, :]], axis=0)
        else:
            low = array[row - 1 : row + ROWS - 1, :]
        if row + ROWS == edge:
            high = jnp.concatenate([array[row + 1 : edge, :], block[ROWS - 1 :, :]], axis=0)
        else:
            high = array[row + 1 : row + ROWS + 1, :]
        return (
            block, low, high,
            behind(block, edge), ahead(block, edge), behind(block, 1), ahead(block, 1),
        )

    for row in range(0, edge, ROWS):
        rows = slice(row, row + ROWS)
        x, _ = iotas((ROWS, lanes))
        outside = (x + row == 0, x + row == edge - 1, first_y, last_y, first_z, last_z)
        k, *around = shifted_rows(coefficient, row)
        v, *beside = shifted_rows(start, row)
        total = None
        sums = None
        for number in range(6):
            face = 0.5 * (k + around[number])
            whole = jnp.where(outside[number], k, face)
            inner = jnp.where(outside[number], 0.0, face)
            for tile in range(lanes // LANES):
                weights[number, tile, rows, :] = inner[:, tiles_of(tile)]
            sums = whole if sums is None else sums + whole
            term = inner * beside[number]
            total = term if total is None else total + term
        sums = 1.0 / (4.0 * sums)
        total = source[rows, :] + 4.0 * total
        for tile in range(lanes // LANES):
            inverse[tile, rows, :] = sums[:, tiles_of(tile)]
            base[tile, rows, :] = total[:, tiles_of(tile)]
    ghosts[...] = select_ghosts(edge, lanes)
    planes[...] = select_planes(edge)
    both[...] = select_both_halves(edge)
    low_half[...] = select_low_half(edge)
    coarsen[...] = coarsening(edge, 4 * LANES, LANES)
    refine[...] = refining(edge, LANES, 4 * LANES)


def fine_kernel(
    groups_x, groups_y, position, colours, faces, source, coefficient, start,
    weights, inverse, base_terms, ghosts, planes_grown, coarsen,
    smoothed, slots,
    ghost, values, kept,
):
    edge = source.shape[0]
    half = edge // 2
    lanes = source.shape[1]
    me = lax.axis_index("gx") * groups_y + lax.axis_index("gy")
    owner, octant = place(position, me, groups_y)
    octant_x = octant // 4
    leading = colours[0:1, 0:1]
    span = half * edge
    tiles = span // LANES

    base = faces[owner]
    sides = select_dot(base[0:half, 0 : 4 * half], ghosts[...])
    double_rows(ghost, sides)
    before = faces[jnp.maximum(owner - 1, 0)][half:, :]
    after = faces[jnp.minimum(owner + 1, groups_x - 1)][half:, :]
    base = base[half:, :]
    before = jnp.where(owner > 0, before, 0.0)
    after = jnp.where(owner < groups_x - 1, after, 0.0)
    line, _ = iotas(base.shape)
    planes = jnp.where(
        line < tiles,
        jnp.where(octant_x == 0, before, base),
        jnp.where(octant_x == 1, after, base),
    )
    planes = jnp.concatenate([planes, planes], axis=0)
    grown = select_dot(planes, planes_grown[...])
    for tile in range(tiles):
        for part in range(2):
            at = 2 * tile + part
            extra = grown[:, part * LANES : (part + 1) * LANES]
            ghost[at, 0:1, :] = ghost[at, 0:1, :] + extra[tile : tile + 1, :]
            ghost[at, edge - 1 : edge, :] = (
                ghost[at, edge - 1 : edge, :] + extra[tiles + tile : tiles + tile + 1, :]
            )
    every = range(lanes // LANES)


    leads = cell_parity(edge) == leading
    row_zero = jnp.zeros((1, LANES), F32)
    for tile in every:
        values[tile, ROWS - 1 : ROWS, :] = row_zero
        values[tile, edge + ROWS : edge + ROWS + 1, :] = row_zero
    for row in range(0, edge, ROWS):
        rows = slice(row, row + ROWS)
        for tile in every:
            lane = tiles_of(tile)
            extra = 4.0 * coefficient[rows, lane] * ghost[tile, rows, :]
            values[tile, row + ROWS : row + 2 * ROWS, :] = jnp.where(
                leads, (base_terms[tile, rows, :] + extra) * inverse[tile, rows, :],
                start[rows, lane],
            )
            kept[tile, rows, :] = source[rows, lane] + extra
    for row in range(0, edge, ROWS):
        rows = slice(row, row + ROWS)
        own, sums = coupled(weights, rows, values, every, row + ROWS, edge)
        for tile in every:
            smoothed[rows, tiles_of(tile)] = jnp.where(
                leads, own[tile],
                (kept[tile, rows, :] + 4.0 * sums[tile]) * inverse[tile, rows, :],
            )
    for tile in every:
        values[tile, ROWS : edge + ROWS, :] = smoothed[:, tiles_of(tile)]
    for row in range(0, edge, ROWS):
        rows = slice(row, row + ROWS)
        own, sums = coupled(weights, rows, values, every, row + ROWS, edge)
        for tile in every:
            ghost[tile, rows, :] = jnp.where(
                leads,
                (source[rows, tiles_of(tile)] - base_terms[tile, rows, :]) + 4.0 * sums[tile],
                0.0,
            )
    chosen = coarsen[...]
    for part in range(lanes // (4 * LANES)):
        block = jnp.concatenate(
            [pair_rows(ghost, 4 * part + tile, 0, half) for tile in range(4)], axis=1
        )
        mean = 0.25 * select_dot(block, chosen)
        for holder in range(groups_x):
            slots[holder, :, part * LANES : (part + 1) * LANES] = mean


def coarse_kernel(
    groups_x, groups_y, position, colours, arrived, residual, start, coefficient,
    y_even, y_odd, from_even, from_odd, both, coarsen,
    source_b, coefficient_b, correction, even_packet, odd_packet,
    grown, kext, comp, extra_v, weights, inverse, first_values, second_values, left,
):
    edge = start.shape[0]
    half = edge // 2
    lanes = start.shape[1]
    span = half * edge
    unit = LANES
    me = lax.axis_index("gx")
    mine_y = lax.axis_index("gy")
    count = lanes // unit
    wide = lanes + 2 * unit
    body = lanes + wide
    rows_all = 2 * edge
    top = half + ROWS
    every = range(count)
    tiles = range(count + 2)

    k_low, k_high = two_sides(mine_y, groups_y, y_even[:, unit:], y_odd[:, unit:])
    kext[0, top : top + edge, :] = k_low
    kext[count + 1, top : top + edge, :] = k_high
    for tile in every:
        kext[tile + 1, top : top + edge, :] = coefficient[:, tiles_of(tile)]
        comp[tile, half : half + edge, :] = residual[tile]

    def unpack(block, there, k_rows, c_rows, k_row, number):
        for tile in every:
            comp[tile, c_rows, :] = jnp.where(there, block[:, tiles_of(tile)], 0.0)
        for tile in tiles:
            kext[tile, k_rows, :] = jnp.where(there, block[:, tiles_of(count + tile)], 0.0)
        for piece in range(body // unit):
            spot = body + piece // half * unit
            line = piece % half
            value = jnp.where(there, block[line : line + 1, spot : spot + unit], 0.0)
            if piece < count:
                extra_v[number : number + 1, tiles_of(piece)] = value
            else:
                kext[piece - count, k_row : k_row + 1, :] = value

    for parity in range(2):
        above, below = (from_even, from_odd) if parity == 0 else (from_odd, from_even)

        @pl.when(me % 2 == parity)
        def _(above=above, below=below):
            unpack(below, me > 0, slice(ROWS, top), slice(0, half), ROWS - 1, 0)
            last = top + edge
            unpack(
                above, me < groups_x - 1, slice(last, last + half),
                slice(half + edge, rows_all), last + half, 1,
            )

    for number, mine, theirs in ((0, half, half - 1), (1, half + edge - 1, half + edge)):
        for tile in every:
            v = start[mine - half : mine - half + 1, tiles_of(tile)]
            k = kext[tile + 1, mine + ROWS : mine + ROWS + 1, :]
            k_other = kext[tile + 1, theirs + ROWS : theirs + ROWS + 1, :]
            flux = (k + k_other) * (v - extra_v[number : number + 1, tiles_of(tile)])
            comp[tile, mine : mine + 1, :] = comp[tile, mine : mine + 1, :] - flux
            comp[tile, theirs : theirs + 1, :] = comp[tile, theirs : theirs + 1, :] + flux

    chosen = both[...]
    for part in range(arrived.shape[2] // unit):
        flat_rows = arrived[:, :, tiles_of(part)].reshape(groups_x * half, unit)
        wider = select_dot(flat_rows, chosen)
        for piece in range(2):
            grown[2 * part + piece] = wider[:, tiles_of(piece)]
    _, lane = iotas((half, unit))
    half_of = lane % edge // half
    for holder in range(groups_x):
        owner, octant = place(position, holder * groups_y + mine_y, groups_y)
        block = 2 * (owner - me) + octant // 4 + 1

        @pl.when((block >= 0) & (block < 4))
        def _(holder=holder, octant=octant, block=block):
            rows = pl.ds(pl.multiple_of(block * half, half), half)
            here = half_of == octant % 2
            for tile in range(span // unit):
                goes = octant // 2 % 2 * (span // unit) + tile
                comp[goes, rows, :] = jnp.where(
                    here, grown[tile, holder * half : (holder + 1) * half, :], comp[goes, rows, :]
                )

    zeros = jnp.zeros((ROWS, unit), F32)
    for ref in (first_values, second_values):
        for tile in tiles:
            ref[tile, 0:ROWS, :] = zeros
            ref[tile, ROWS + rows_all :, :] = zeros
    leads = cell_parity(edge) == colours[0:1, 1:2]
    y_there = {0: mine_y > 0, count + 1: mine_y < groups_y - 1}
    for row in range(0, rows_all, ROWS):
        at = row + ROWS
        rows = slice(row, row + ROWS)
        w, diagonals = twice_faces(*six_around(kext, tiles, at, edge), edge)
        x_there = None
        if row < half:
            x_there = me > 0
        elif row >= half + edge:
            x_there = me < groups_x - 1
        for tile in tiles:
            for number in range(6):
                weights[number, tile, rows, :] = w[tile][number]
            inv = 1.0 / diagonals[tile]
            for there in (x_there, y_there.get(tile)):
                if there is not None:
                    inv = jnp.where(there, inv, 0.0)
            inverse[tile, rows, :] = inv
            if tile in y_there:
                first_values[tile, at : at + ROWS, :] = zeros
            else:
                first_values[tile, at : at + ROWS, :] = jnp.where(
                    leads, comp[tile - 1, rows, :] * inv, 0.0
                )

    for row in range(0, rows_all, ROWS):
        rows = slice(row, row + ROWS)
        at = row + ROWS
        own, sums = coupled(weights, rows, first_values, tiles, at, edge)
        for tile in tiles:
            total = sums[tile]
            if tile not in y_there:
                total = total + comp[tile - 1, rows, :]
            total = jnp.where(leads, 0.0, total * inverse[tile, rows, :])
            second_values[tile, at : at + ROWS, :] = total
            if half <= row < half + edge and tile not in y_there:
                correction[row - half : row - half + ROWS, tiles_of(tile - 1)] = own[tile] + total
    for row in range(0, rows_all, ROWS):
        rows = slice(row, row + ROWS)
        own, sums = coupled(weights, rows, second_values, tiles, row + ROWS, edge)
        for tile in tiles:
            left[tile, rows, :] = jnp.where(leads, sums[tile], 0.0)

    chosen = coarsen[...]

    def pairs(ref, these, first):
        return jnp.concatenate([pair_rows(ref, tile, first, edge) for tile in these], axis=1)

    blocks = count // 4
    source_b[:, 0:unit] = 0.0625 * select_dot(pairs(left, [0], 0), chosen[3 * unit :, :])
    source_b[:, (blocks + 1) * unit :] = 0.0625 * select_dot(
        pairs(left, [count + 1], 0), chosen[0:unit, :]
    )
    for part in range(blocks):
        these = range(4 * part + 1, 4 * part + 5)
        source_b[:, tiles_of(part + 1)] = 0.0625 * select_dot(pairs(left, these, 0), chosen)
        coefficient_b[:, tiles_of(part)] = 0.125 * select_dot(pairs(kext, these, ROWS), chosen)
    middle = (blocks + 2) // 2 * unit
    rows = slice(ROWS + half, ROWS + half + edge)
    for parity in range(2):
        up, down = (even_packet, odd_packet) if parity == 0 else (odd_packet, even_packet)

        @pl.when(mine_y % 2 == parity)
        def _(up=up, down=down):
            up[:, 0:middle] = source_b[:, middle:]
            up[:, middle : middle + unit] = coefficient_b[:, (blocks - 1) * unit :]
            up[:, middle + unit :] = second_values[count + 1, rows, :]
            down[:, 0:middle] = source_b[:, 0:middle]
            down[:, middle : middle + unit] = coefficient_b[:, 0:unit]
            down[:, middle + unit :] = second_values[0, rows, :]


def bottom_kernel(
    groups_x, groups_y, position, colours, source_b, coefficient_b, correction,
    from_even, from_odd, low_half, refine,
    corrected, slots,
    spread, table, low, high,
):
    edge = correction.shape[0]
    half = edge // 2
    lanes = correction.shape[1]
    span = half * edge
    unit = LANES
    me = lax.axis_index("gx")
    mine_y = lax.axis_index("gy")
    low[...], high[...] = two_sides(mine_y, groups_y, from_even[...], from_odd[...])
    middle = source_b.shape[1] // 2
    count = 2 * middle // unit
    f_bottom = []
    k_bottom = []
    for tile in range(count):
        side, at = (low, tile) if tile < count // 2 else (high, tile - count // 2)
        f_bottom.append(source_b[:, tiles_of(tile)] + side[:, tiles_of(at)])
        if tile == 0:
            k_bottom.append(low[:, middle : middle + unit])
        elif tile == count - 1:
            k_bottom.append(high[:, middle : middle + unit])
        else:
            k_bottom.append(coefficient_b[:, tiles_of(tile - 1)])
    quarter = half // 2

    def around(tiles):
        return (
            [pltpu.roll(one, 1, 0) for one in tiles],
            [pltpu.roll(one, edge - 1, 0) for one in tiles],
        ) + along_y(tiles, half) + along_z(tiles)

    w, diagonals = twice_faces(k_bottom, around(k_bottom), half)
    x, lane = iotas((edge, unit))
    x = x + (me * half - quarter)
    x_there = (x >= 0) & (x < groups_x * half)
    first = colours[0:1, 2:3]
    parity = (x + lane // half + lane % half) % 2
    scaled = []
    shares = []
    for tile in range(count):
        inv = 1.0 / diagonals[tile]
        there = x_there
        if tile == 0:
            there = there & (mine_y > 0)
        if tile == count - 1:
            there = there & (mine_y < groups_y - 1)
        inv = jnp.where(there, inv, 0.0)
        shares.append([jnp.where(parity == c, inv, 0.0) for c in (first, 1 - first)])
        scaled.append([8.0 * f_bottom[tile] * one for one in shares[tile]])
    values = [[one[0] for one in scaled], None]
    for step in range(1, 2 * SWEEPS):
        colour = step % 2
        beside = around(values[1 - colour])
        fresh = []
        for tile in range(count):
            total = w[tile][0] * beside[0][tile]
            for number in range(1, 6):
                total = total + w[tile][number] * beside[number][tile]
            fresh.append(scaled[tile][colour] + total * shares[tile][colour])
        values[colour] = fresh
    bottom = [one + other for one, other in zip(*values)]

    chosen = refine[...]
    for part in range(lanes // (4 * unit)):
        block = bottom[part + 1][quarter : quarter + half, :]
        double_rows(spread.at[pl.ds(4 * part, 4)], select_dot(block, chosen))
    every = range(lanes // unit)
    for row in range(0, edge, ROWS):
        rows = slice(row, row + ROWS)
        total = correction[rows, :] + flat(spread, rows, every)
        ring = [total[:, tiles_of(tile)] for tile in every]
        ring[0] = ring[0] + low[rows, middle + unit :]
        ring[-1] = ring[-1] + high[rows, middle + unit :]
        total = jnp.concatenate(ring, axis=1)
        corrected[rows, :] = total

    chosen = low_half[...]
    for octant_x in range(2):
        for octant_y in range(2):
            block = corrected[
                octant_x * half : (octant_x + 1) * half,
                octant_y * span : (octant_y + 1) * span,
            ]
            if (octant_x + octant_y) % 2 == 1:
                block = ahead(block, half)
            for part in range(span // (2 * unit)):
                table[2 * octant_x + octant_y, :, part * unit : (part + 1) * unit] = select_dot(
                    block[:, part * 2 * unit : (part + 1) * 2 * unit], chosen
                )
    for holder in range(groups_x):
        _, octant = place(position, holder * groups_y + mine_y, groups_y)
        slots[holder] = table[octant // 4 * 2 + octant // 2 % 2]


def finish_kernel(
    groups_y, position, arrived, smoothed, start, correction, refine,
    coarse_out, out, grown,
):
    edge = smoothed.shape[0]
    me = lax.axis_index("gx") * groups_y + lax.axis_index("gy")
    owner, _ = place(position, me, groups_y)
    coarse_out[...] = start[...] + correction[...]
    value = arrived[owner]
    chosen = refine[...]
    for part in range(value.shape[1] // LANES):
        fine = select_dot(value[:, tiles_of(part)], chosen)
        double_rows(grown.at[pl.ds(4 * part, 4)], fine)
    out[...] = smoothed[...] + flat(grown, slice(0, edge), range(smoothed.shape[1] // LANES))


def call(kernel, outs, scratch, specs, *operands):
    return pl.pallas_call(
        kernel,
        out_shape=[jax.ShapeDtypeStruct(shape, F32) for shape in outs],
        in_specs=specs,
        out_specs=[VMEM] * len(outs),
        scratch_shapes=[pltpu.VMEM(shape, F32) for shape in scratch],
        compiler_params=PARAMS,
    )(*operands)


def tiled(rows, lanes):
    return (lanes // LANES, rows, LANES)


def matching(axis, first):
    sizes = (lax.axis_size("gx"), lax.axis_size("gy"))
    along_x = axis == "gx"
    size, others = sizes if along_x else sizes[::-1]
    pairs = []
    for other in range(others):
        for i in range(size):
            j = i + 1 if (i - first) % 2 == 0 else i - 1
            goes, beside = j, other
            if not 0 <= j < size:
                goes, beside = i, other ^ 1
            if beside < others:
                here, there = (i, other), (goes, beside)
                if not along_x:
                    here, there = here[::-1], there[::-1]
                pairs.append((here[0] * sizes[1] + here[1], there[0] * sizes[1] + there[1]))
    return pairs


def swapped(even_packet, odd_packet, axis):
    return tuple(
        lax.ppermute(packet, ("gx", "gy"), matching(axis, first))
        for first, packet in ((0, even_packet), (1, odd_packet))
    )


def on_device(
    coarse_source,
    coarse_coefficient,
    coarse_start,
    fine_source,
    fine_coefficient,
    fine_start,
    fine_position,
    first_colour,
):
    groups_x = lax.axis_size("gx")
    groups_y = lax.axis_size("gy")
    edge, lanes = coarse_source.shape
    half = edge // 2
    span = half * edge
    compact = half * half
    wide = lanes + 2 * LANES
    positions = fine_position.reshape(1, -1)
    colours = first_colour.reshape(1, -1)
    even_packet, odd_packet, positions, colours, faces_0, faces_1 = pl.pallas_call(
        border_kernel,
        out_shape=[jax.ShapeDtypeStruct((edge, 2 * LANES), F32)] * 2
        + [jax.ShapeDtypeStruct(array.shape, array.dtype) for array in (positions, colours)]
        + [jax.ShapeDtypeStruct((span + 2 * LANES, LANES), BF16)] * 2,
        in_specs=[HBM] * 4,
        out_specs=[VMEM] * 6,
        scratch_shapes=[pltpu.SemaphoreType.DMA((6,))],
        compiler_params=PARAMS,
    )(coarse_start, coarse_coefficient, positions, colours)
    y_even, y_odd = swapped(even_packet, odd_packet, "gy")
    face_rows = half + 2 * (span // LANES)
    (slots,) = call(
        functools.partial(faces_kernel, groups_x, groups_y),
        [(groups_x, face_rows, LANES)],
        [(8, face_rows, LANES), (edge, LANES), (edge, LANES)],
        [VMEM] * 7,
        positions, colours, coarse_start, y_even, y_odd, faces_0, faces_1,
    )
    faces = lax.all_to_all(slots, "gx", 0, 0, tiled=True)
    _, y_even, y_odd = lax.optimization_barrier((slots, y_even, y_odd))
    extra = -(-(lanes + wide) // LANES // half) * LANES
    packed = lanes + wide + extra
    residual, even_packet, odd_packet = call(
        functools.partial(residual_kernel, groups_y),
        [tiled(edge, lanes), (half, packed), (half, packed)],
        [tiled(edge + 2 * ROWS, wide)] * 2 + [(edge, 2 * LANES)] * 2,
        [VMEM] * 5,
        coarse_start, coarse_coefficient, coarse_source, y_even, y_odd,
    )
    from_even, from_odd = swapped(even_packet, odd_packet, "gx")
    box = (fine_source[0], fine_coefficient[0], fine_start[0])
    weights, inverse, base, ghosts, planes, both, low_half, coarsen, refine = pl.pallas_call(
        box_terms_kernel,
        out_shape=[
            jax.ShapeDtypeStruct(shape, F32)
            for shape in [(6,) + tiled(edge, lanes), tiled(edge, lanes), tiled(edge, lanes)]
        ]
        + [
            jax.ShapeDtypeStruct(shape, BF16)
            for shape in [
                (4 * half, lanes),
                (LANES, 2 * LANES),
                (LANES, 2 * LANES),
                (2 * LANES, LANES),
                (4 * LANES, LANES),
                (LANES, 4 * LANES),
            ]
        ],
        in_specs=[VMEM] * 3,
        out_specs=[VMEM] * 9,
        compiler_params=PARAMS,
    )(*box)
    smoothed, restricted = call(
        functools.partial(fine_kernel, groups_x, groups_y),
        [(edge, lanes), (groups_x, half, compact)],
        [tiled(edge, lanes), tiled(edge + 2 * ROWS, lanes), tiled(edge, lanes)],
        [VMEM] * 12,
        positions, colours, faces, *box, weights, inverse, base, ghosts, planes, coarsen,
    )
    arrived = lax.all_to_all(restricted, "gx", 0, 0, tiled=True)
    rows = 2 * edge
    lanes_b = (wide // LANES - 2) // 4 * LANES
    source_b, coefficient_b, correction, even_packet, odd_packet = call(
        functools.partial(coarse_kernel, groups_x, groups_y),
        [
            (edge, lanes_b + 2 * LANES),
            (edge, lanes_b),
            (edge, lanes),
            (edge, lanes_b // 2 + 3 * LANES),
            (edge, lanes_b // 2 + 3 * LANES),
        ],
        [
            (span // LANES, groups_x * half, LANES),
            tiled(rows + 2 * ROWS, wide),
            tiled(rows, lanes),
            (ROWS, lanes),
            (6,) + tiled(rows, wide),
            tiled(rows, wide),
            tiled(rows + 2 * ROWS, wide),
            tiled(rows + 2 * ROWS, wide),
            tiled(rows, wide),
        ],
        [VMEM] * 12,
        positions, colours, arrived, residual, coarse_start, coarse_coefficient,
        y_even, y_odd, from_even, from_odd, both, coarsen,
    )
    y_even, y_odd = swapped(even_packet, odd_packet, "gy")
    corrected, slots = call(
        functools.partial(bottom_kernel, groups_x, groups_y),
        [(edge, lanes), (groups_x, half, compact)],
        [tiled(edge, lanes), (4, half, compact)]
        + [(edge, lanes_b // 2 + 3 * LANES)] * 2,
        [VMEM] * 9,
        positions, colours, source_b, coefficient_b, correction, y_even, y_odd, low_half, refine,
    )
    returned = lax.all_to_all(slots, "gx", 0, 0, tiled=True)
    coarse_solution, fine_solution = call(
        functools.partial(finish_kernel, groups_y),
        [(edge, lanes), (edge, lanes)],
        [tiled(edge, lanes)],
        [VMEM] * 6,
        positions, returned, smoothed, coarse_start, corrected, refine,
    )
    return (coarse_solution, fine_solution[None])


def solution(mesh):
    placed = (
        P("gx", "gy"),
        P("gx", "gy"),
        P("gx", "gy"),
        P(("gx", "gy"), None, None),
        P(("gx", "gy"), None, None),
        P(("gx", "gy"), None, None),
        P(),
        P(),
    )

    return jax.shard_map(
        on_device,
        mesh=mesh,
        in_specs=placed,
        out_specs=(P("gx", "gy"), P(("gx", "gy"), None, None)),
        check_vma=False,
    )
```
